256 devices in a mesh: layer: 32 (over x, z), row: 2 (over core), col: 4 (over y).
Axes of the slice: x: 4, y: 4, z: 8, core: 2. Of those that a mesh axis runs over, the one named last changes fastest.
Arguments:
- inputs: float32 [1, 4, 384, 128], P(None, 'row', 'col'), may hold values from -6 to 6
- weights: float32 [256, 9, 128, 128], P('layer'), may hold values from -0.1875 to 0.1875
- biases: float32 [256, 128], P('layer'), may hold values from -3 to 3
Outputs:
- states: float32 [256, 1, 4, 384, 128], P('layer', None, 'row', 'col')
The draws below stay inside these ranges and needn't reach their ends.
All inputs are finite; a program needn't handle non-finite values.
Results may differ from the reference program's by a relative error of at most 0.0003.
Values sent between devices are 32-bit elements; how exact they have to be, the bound alone decides.
A program may use at most 64 MiB of HBM per device.

```python
import jax
import jax.numpy as jnp
from jax import lax

CHANNELS = 128
SEC_LAYERS = 8
CYCLES = 2
BATCH = 1
SECTIONS = 32
LAYERS = 256
HEIGHT = 4
WIDTH = 384


def block_levels(key, shape, split, least, top_value):
    gain, own = 1.0, jax.random.fold_in(key, 6)
    for axis_at, parts in split:
        heights = jnp.exp(jax.random.uniform(jax.random.fold_in(own, axis_at), (parts,), jnp.float32, least / len(split), top_value / len(split)))
        gain = gain * jnp.repeat(heights, shape[axis_at] // parts).reshape([-1 if axis == axis_at else 1 for axis in range(len(shape))])
    return gain


def gaussian(own_key, shape, deviation, most, split=(), kind=jnp.bfloat16):
    result = jax.random.normal(own_key, shape, jnp.float32) * deviation
    if len(split) > 0:
        result = block_levels(own_key, shape, split, -0.22, 0.18) * result
    return jnp.clip(result, min=-most, max=most).astype(kind)


def setup_inputs(seed: int = 0) -> dict:
    key_list = jax.random.split(jax.random.key(seed), 4)
    inputs = gaussian(key_list[0], (BATCH, HEIGHT, WIDTH, CHANNELS), 1.0, 6.0, ((1, 2), (2, 4)), jnp.float32)
    weights = gaussian(key_list[1], (LAYERS, 9, CHANNELS, CHANNELS), (9 * CHANNELS) ** -0.5, 0.1875, ((0, 32),), jnp.float32)
    biases = gaussian(key_list[2], (LAYERS, CHANNELS), 0.5, 3.0, ((0, 32),), jnp.float32)
    return {"inputs": inputs, "weights": weights, "biases": biases}


step_size = 0.2


def advance(current, weight, bias_row):
    padded = jnp.pad(current, ((0, 0), (1, 1), (1, 1), (0, 0)))
    row_count = current.shape[1]
    col_count = current.shape[2]
    channel_count = current.shape[3]
    stacked = jnp.concatenate([padded[:, row_off:row_off + row_count, col_off:col_off + col_count, :] for row_off in range(3) for col_off in range(3)], axis=-1)
    preact = jnp.dot(stacked.reshape(-1, 9 * channel_count), weight.reshape(9 * channel_count, channel_count), precision=lax.Precision.HIGHEST, preferred_element_type=jnp.float32)
    return current + step_size * jnp.tanh(preact.reshape(current.shape) + bias_row)


def affine(field, matrix):
    return jnp.dot(field.reshape(-1, matrix.shape[0]), matrix, precision=lax.Precision.HIGHEST, preferred_element_type=jnp.float32).reshape(field.shape)


def sweep(segment_items):
    start, weight, bias_rows = segment_items
    current = start
    inner_states = []
    for layer_idx in range(SEC_LAYERS - 1):
        current = advance(current, weight[layer_idx], bias_rows[layer_idx])
        inner_states.append(current)
    ending = advance(current, weight[SEC_LAYERS - 1], bias_rows[SEC_LAYERS - 1])
    return jnp.stack(inner_states), ending


def reference(inputs, weights, biases):
    sec_weights = weights.reshape(SECTIONS, SEC_LAYERS, 9, CHANNELS, CHANNELS)
    sec_biases = biases.reshape(SECTIONS, SEC_LAYERS, CHANNELS)
    coarse_maps = jnp.eye(CHANNELS, dtype=jnp.float32) + step_size * jnp.sum(sec_weights, axis=(1, 2))
    coarse = jnp.broadcast_to(inputs, (SECTIONS,) + inputs.shape)

    def starts_of(values):
        return jnp.concatenate([inputs[None], values[:-1]], axis=0)

    def run_all(starts):
        return lax.map(sweep, (starts, sec_weights, sec_biases))

    def solve_segment(previous, segment_items):
        correction, matrix = segment_items
        updated = affine(previous, matrix) + correction
        return updated, updated

    for cycle_idx in range(CYCLES):
        unused, coarse = run_all(starts_of(coarse))
        starts = starts_of(coarse)
        unused, endings = run_all(starts)
        corrections = endings - jax.vmap(affine)(starts, coarse_maps)
        unused, coarse = lax.scan(solve_segment, inputs, (corrections, coarse_maps))
    inner_states, unused = run_all(starts_of(coarse))
    combined = jnp.concatenate([inner_states, coarse[:, None]], axis=1)
    return combined.reshape((LAYERS,) + inputs.shape)
```

```python
import jax
import jax.numpy as jnp
from jax import lax
from jax.experimental import pallas as pl
from jax.experimental.pallas import tpu as pltpu
from jax.sharding import PartitionSpec as P

MESH = pl.DeviceIdType.MESH
F32, BF16 = jnp.float32, jnp.bfloat16
CYCLES = 2
STEP = 0.2
X, Z = 4, 8
CH = 128
LAY = 8
H = 4
TC = 48
TW = TC + 2 * LAY
PX = H * TW
SH = H * TC // Z


def split(a):
    high = a.astype(BF16).astype(F32)
    return high, a - high


def paired(a):
    high, low = split(a)
    return jnp.concatenate([high, low], axis=1).astype(BF16)


def fold(r, m):
    return (r[:m, :CH] + r[:m, CH:]) + (r[m:, :CH] + r[m:, CH:])


def times(a, pair):
    high, low = split(a)
    stacked = jnp.concatenate([high, low], axis=0).astype(BF16)
    r = jnp.dot(stacked, pair, preferred_element_type=F32)
    return fold(r, a.shape[0])


def kernel(
    inp, wts, bias, out,
    xin, x0, wf, wc, psum, a_buf, pad, mask, st, cc, rs, rz, bz, dp, tx, tb, pz, mx, mown, pc, qc, sc, nc, outb,
    s_in, r_in, w_sem, s_sh, r_sh, s_p, r_p, s_pf, r_pf, s_m, r_m, s_a, r_a, s_t, r_t, s_b, r_b,
    s_h, r_h, s_o, r_o, l_o, x_sem,
):
    sec = lax.axis_index("layer")
    r = lax.axis_index("row")
    c = lax.axis_index("col")
    ncol = lax.axis_size("col")
    x, z = sec // Z, sec % Z
    t = 2 * c + r
    last = 2 * ncol - 1

    def at(layer, row, col):
        return {"layer": layer, "row": row, "col": col}

    def remote(src, dst, ss, rr, dev):
        return pltpu.make_async_remote_copy(
            src_ref=src, dst_ref=dst, send_sem=ss, recv_sem=rr, device_id=dev, device_id_type=MESH
        )

    right_rc = (1 - r, c + r)
    left_rc = (1 - r, c - (1 - r))
    has_right, has_left = t < last, t > 0

    load_x = pltpu.make_async_copy(inp.at[0], xin, x_sem.at[0])
    load_x.start()

    def load_w(l):
        return pltpu.make_async_copy(wts.at[l], wf.at[l], w_sem.at[l])

    for l in range(LAY):
        load_w(l).start()

    bar = pltpu.get_barrier_semaphore()

    def greet(dev):
        pl.semaphore_signal(bar, inc=1, device_id=dev, device_id_type=MESH)

    for k in range(1, Z):
        greet(at(x * Z + (z + k) % Z, r, c))
    for k in range(1, X):
        greet(at(((x + k) % X) * Z + z, r, c))

    up = (z == Z - 1) & (x < X - 1)
    down = (z == 0) & (x > 0)

    @pl.when(up)
    def _():
        greet(at(sec + 1, r, c))

    @pl.when(down)
    def _():
        greet(at(sec - 1, r, c))

    for ok, (rr, c2) in ((has_right, right_rc), (has_left, left_rc)):
        @pl.when(ok)
        def _():
            for k in range(Z):
                greet(at(x * Z + k, rr, c2))

            @pl.when(up)
            def _():
                greet(at(sec + 1, rr, c2))

            @pl.when(down)
            def _():
                greet(at(sec - 1, rr, c2))

    @pl.when(c < ncol - 1)
    def _():
        greet(at(sec, r, c + 1))

    @pl.when(c > 0)
    def _():
        greet(at(sec, r, c - 1))

    one = lambda cond: jnp.where(cond, 1, 0)
    sides = one(has_right) + one(has_left)
    peers = (Z - 1) + (X - 1) + sides * Z + (1 + sides) * (one(up) + one(down)) + one(c < ncol - 1) + one(c > 0)

    zero_cols = jnp.zeros((H, LAY, CH), F32)

    @pl.when(t == 0)
    def _():
        x0[:, 0:LAY, :] = zero_cols
        for i in range(CYCLES):
            st[i, :, 0:LAY, :] = zero_cols
            dp[i, :, 0:LAY, :] = zero_cols

    @pl.when(t == last)
    def _():
        x0[:, TW - LAY : TW, :] = zero_cols
        for i in range(CYCLES):
            st[i, :, TW - LAY : TW, :] = zero_cols
            dp[i, :, TW - LAY : TW, :] = zero_cols

    a_buf[...] = jnp.zeros_like(a_buf)
    pad[...] = jnp.zeros_like(pad)
    psum[...] = jnp.zeros_like(psum)
    column = lax.broadcasted_iota(jnp.int32, (H, TW, CH), 1)
    inside = ((column >= LAY) | (t > 0)) & ((column < TW - LAY) | (t < last))
    mask[...] = jnp.where(inside, 1.0, 0.0).astype(F32).reshape(PX, CH)

    pl.semaphore_wait(bar, peers)
    load_x.wait()

    wide = TC + LAY
    half = pl.ds(2 * r, 2)
    mine = pl.ds(pl.multiple_of(LAY * (1 - r), LAY), wide)
    theirs = pl.ds(pl.multiple_of(LAY * r, LAY), wide)
    src_mine = pl.ds(pl.multiple_of((TC - LAY) * r, LAY), wide)
    src_theirs = pl.ds(pl.multiple_of((TC - LAY) * (1 - r), LAY), wide)
    to_core = remote(xin.at[:, src_theirs, :], x0.at[half, theirs, :], s_in.at[0], r_in.at[0], at(sec, 1 - r, c))
    to_right = remote(
        xin.at[:, pl.ds(2 * TC - LAY, LAY), :], x0.at[half, pl.ds(0, LAY), :], s_in.at[1], r_in.at[1 + r], at(sec, 0, c + 1)
    )
    to_left = remote(
        xin.at[:, pl.ds(0, LAY), :], x0.at[half, pl.ds(TW - LAY, LAY), :], s_in.at[2], r_in.at[3 + r], at(sec, 1, c - 1)
    )
    to_core.start()

    @pl.when(c < ncol - 1)
    def _():
        to_right.start()

    @pl.when(c > 0)
    def _():
        to_left.start()

    x0[half, mine, :] = xin[:, src_mine, :]

    def got_in(i, cols):
        part = x0.at[pl.ds(0, 2), cols, :]
        return remote(part, part, s_in.at[0], r_in.at[i], at(sec, 1 - r, c))

    got_in(0, pl.ds(0, wide)).wait_recv()

    @pl.when((r == 0) & (c > 0))
    def _():
        got_in(1, pl.ds(0, LAY)).wait_recv()
        got_in(2, pl.ds(0, LAY)).wait_recv()

    @pl.when((r == 1) & (c < ncol - 1))
    def _():
        got_in(3, pl.ds(0, LAY)).wait_recv()
        got_in(4, pl.ds(0, LAY)).wait_recv()

    to_core.wait_send()

    @pl.when(c < ncol - 1)
    def _():
        to_right.wait_send()

    @pl.when(c > 0)
    def _():
        to_left.wait_send()

    def set_start(value):
        pad[LAY : LAY + PX, :] = value.reshape(PX, CH)

    def layer(l):
        v = pad[LAY : LAY + PX, :]
        for d in range(3):
            high, low = split(pad[LAY - 1 + d : LAY - 1 + d + PX, :])
            a_buf[0, TW : TW + PX, d * CH : (d + 1) * CH] = high.astype(BF16)
            a_buf[1, TW : TW + PX, d * CH : (d + 1) * CH] = low.astype(BF16)
        lhs = jnp.concatenate(
            [
                jnp.concatenate([a_buf[h, d * TW : d * TW + PX, :] for d in range(3)], axis=1)
                for h in range(2)
            ],
            axis=0,
        )
        pre = fold(jnp.dot(lhs, wc[l], preferred_element_type=F32), PX)
        new = (v + STEP * jnp.tanh(pre + bias[pl.ds(l, 1), :])) * mask[...]
        pad[LAY : LAY + PX, :] = new
        return new

    def core(value):
        return value.reshape(H, TW, CH)[:, LAY : LAY + TC, :]

    set_start(x0[...])

    def first(l, carry):
        load_w(l).wait()
        total = psum[...]
        for k in range(9):
            w = wf[l, k]
            total = total + w
            wc[l, k * CH : (k + 1) * CH, :] = paired(w)
        psum[...] = total
        layer(l)
        return carry

    def plain(l, carry):
        layer(l)
        return carry

    lax.fori_loop(0, LAY, first, 0)
    rows_i = lax.broadcasted_iota(jnp.int32, (CH, CH), 0)
    cols_i = lax.broadcasted_iota(jnp.int32, (CH, CH), 1)
    eye = jnp.where(rows_i == cols_i, 1.0, 0.0).astype(F32)
    psum[...] = eye + STEP * psum[...]

    def shift(i):
        nxt = sec + 1
        main = remote(cc.at[i], st.at[i, :, pl.ds(LAY, TC), :], s_sh.at[i, 0], r_sh.at[i, 0], at(nxt, r, c))
        rgt = remote(
            cc.at[i, :, pl.ds(TC - LAY, LAY), :], st.at[i, :, pl.ds(0, LAY), :], s_sh.at[i, 1], r_sh.at[i, 1], at(nxt, *right_rc)
        )
        lft = remote(
            cc.at[i, :, pl.ds(0, LAY), :], st.at[i, :, pl.ds(TW - LAY, LAY), :], s_sh.at[i, 2], r_sh.at[i, 2], at(nxt, *left_rc)
        )
        return main, rgt, lft

    def shift_send(i):
        main, rgt, lft = shift(i)

        @pl.when(sec < X * Z - 1)
        def _():
            @pl.when(has_right)
            def _():
                rgt.start()

            @pl.when(has_left)
            def _():
                lft.start()

            main.start()

    def shift_wait(i):
        main, rgt, lft = shift(i)

        @pl.when(sec > 0)
        def _():
            main.wait_recv()

            @pl.when(has_left)
            def _():
                rgt.wait_recv()

            @pl.when(has_right)
            def _():
                lft.wait_recv()

        @pl.when(sec == 0)
        def _():
            st[i] = x0[...]

        @pl.when(sec < X * Z - 1)
        def _():
            main.wait_send()

            @pl.when(has_right)
            def _():
                rgt.wait_send()

            @pl.when(has_left)
            def _():
                lft.wait_send()

    hrows = pl.ds(pl.multiple_of(r * (CH // 2), CH // 2), CH // 2)

    def p_copy(k):
        return remote(
            psum.at[hrows, :], pz.at[z, hrows, :], s_p.at[k], r_p.at[k], at(x * Z + (z + k) % Z, r, c)
        )

    def m_copy(k):
        return remote(mown, mx.at[x], s_m.at[k], r_m.at[k], at(((x + k) % X) * Z + z, r, c))

    def a_copy(i, k):
        j = (z + k) % Z
        part = rs.at[i, j // 2, pl.ds(pl.multiple_of(SH * (j % 2), LAY), SH), :]
        return remote(part, rz.at[i, z], s_a.at[i, k], r_a.at[i, k], at(x * Z + j, r, c))

    def t_copy(i, k):
        return remote(tb.at[i], tx.at[i, x], s_t.at[i, k], r_t.at[i, k], at(((x + k) % X) * Z + z, r, c))

    my_cols = pl.ds(pl.multiple_of(LAY + SH * (z % 2), LAY), SH)

    def b_copy(i, k):
        j = (z + k) % Z
        return remote(bz.at[i, j], dp.at[i, z // 2, my_cols, :], s_b.at[i, k], r_b.at[i, k], at(x * Z + j, r, c))

    def h_copy(i, k, side):
        frm = (SH - LAY) if side == 0 else 0
        to = 0 if side == 0 else TW - LAY
        rc = right_rc if side == 0 else left_rc
        return remote(
            bz.at[i, k, pl.ds(frm, LAY), :], dp.at[i, z // 2, pl.ds(to, LAY), :], s_h.at[i, k], r_h.at[i, side, z // 2],
            at(x * Z + k, *rc),
        )

    my_shard = (z // 2, pl.ds(pl.multiple_of(SH * (z % 2), LAY), SH))

    for i in range(CYCLES):
        if i > 0:
            lax.fori_loop(0, LAY, plain, 0)
        cc[i] = core(pad[LAY : LAY + PX, :])
        shift_send(i)
        if i == 0:
            for k in range(1, Z):
                p_copy(k).start()
            pz[z, hrows, :] = psum[hrows, :]
        shift_wait(i)
        set_start(st[i])
        lax.fori_loop(0, LAY, plain, 0)
        rs[i] = core(pad[LAY : LAY + PX, :]) - cc[i]
        for k in (4, 3, 5, 2, 6, 1, 7):
            a_copy(i, k).start()
        rz[i, z] = rs[i, my_shard[0], my_shard[1], :]
        if i == 0:
            for k in range(1, Z):
                p_copy(k).wait()
            forward = remote(pz.at[:, hrows, :], pz.at[:, hrows, :], s_pf.at[0], r_pf.at[0], at(sec, 1 - r, c))
            forward.start()
            forward.wait()
            prefix, suffix = pz[0], eye
            for k in range(Z):
                pc[k] = paired(pz[k])
            for k in range(Z):
                if k > 0:
                    prefix = times(prefix, pc[k])
                if k < Z - 1:
                    qc[:, 2 * CH * k : 2 * CH * (k + 1)] = paired(prefix)
                back = Z - 1 - k
                pair = paired(suffix)
                sc[back * CH : (back + 1) * CH, :] = pair
                if back > 0:
                    suffix = times(pz[back], pair)
            mown[...] = prefix
            for k in range(1, X):
                m_copy(k).start()
        for k in range(1, Z):
            a_copy(i, k).wait()
        joined = jnp.concatenate([rz[i, k] for k in range(Z)], axis=1)
        tb[i] = times(joined, sc[...])
        for k in range(1, X):
            t_copy(i, k).start()
        run = rz[i, 0]
        local = [run]
        for k in range(1, Z - 1):
            run = times(run, pc[k]) + rz[i, k]
            local.append(run)
        if i == 0:
            for k in range(1, X):
                m_copy(k).wait()
            near = mx[jnp.maximum(x - 1, 0)]
            far = mx[jnp.maximum(x - 2, 0)]
            near = jnp.where(x >= 2, near, 0.0)
            far = jnp.where(x >= 3, far, 0.0)
            near_pair = paired(near)
            nc[0:CH, :] = near_pair
            nc[CH : 2 * CH, :] = paired(times(far, near_pair))
        for k in range(1, X):
            t_copy(i, k).wait()
        before = [jnp.where(x >= d, tx[i, jnp.maximum(x - d, 0)], 0.0) for d in range(1, X)]
        carry = before[0] + times(jnp.concatenate(before[1:], axis=1), nc[...])
        bz[i, 0] = carry
        high, low = split(carry)
        spread = jnp.dot(jnp.concatenate([high, low], axis=0).astype(BF16), qc[...], preferred_element_type=F32)
        for k in range(1, Z):
            bz[i, k] = local[k - 1] + fold(spread[:, 2 * CH * (k - 1) : 2 * CH * k], SH)
        for k in (4, 3, 5, 2, 6, 1, 7):
            b_copy(i, k).start()

        @pl.when((z % 2 == 1) & has_right)
        def _():
            for k in range(Z):
                h_copy(i, k, 0).start()

        @pl.when((z % 2 == 0) & has_left)
        def _():
            for k in range(Z):
                h_copy(i, k, 1).start()

        dp[i, z // 2, my_cols, :] = bz[i, z]
        for k in range(1, Z):
            b_copy(i, k).wait()

        def halo_in(side, row):
            part = dp.at[i, row, pl.ds(0 if side == 0 else TW - LAY, LAY), :]
            return remote(part, part, s_h.at[i, 0], r_h.at[i, side, row], at(sec, 1 - r, c))

        @pl.when(has_left)
        def _():
            for row in range(H):
                halo_in(0, row).wait_recv()

        @pl.when(has_right)
        def _():
            for row in range(H):
                halo_in(1, row).wait_recv()

        @pl.when((z % 2 == 1) & has_right)
        def _():
            for k in range(Z):
                h_copy(i, k, 0).wait_send()

        @pl.when((z % 2 == 0) & has_left)
        def _():
            for k in range(Z):
                h_copy(i, k, 1).wait_send()

        set_start(st[i] + dp[i])

    out_cols = pl.ds(pl.multiple_of(TC * r, LAY), TC)

    def keep(l):
        return pltpu.make_async_copy(outb.at[l, half], out.at[l, 0, :, out_cols, :], l_o.at[l])

    def give(l):
        return remote(
            outb.at[l, pl.ds(2 * (1 - r), 2)], out.at[l, 0, :, out_cols, :], s_o.at[l], r_o.at[l], at(sec, 1 - r, c)
        )

    i = CYCLES - 1
    delta = times(dp[i, :, pl.ds(LAY, TC), :].reshape(H * TC, CH), paired(psum[...])).reshape(H, TC, CH) + rs[i]
    outb[LAY - 1] = cc[i] + delta
    keep(LAY - 1).start()
    give(LAY - 1).start()

    def final(l, carry):
        outb[l] = core(layer(l))
        keep(l).start()
        give(l).start()
        return carry

    lax.fori_loop(0, LAY - 1, final, 0)
    for l in range(LAY):
        keep(l).wait()
        give(l).wait()


def shards(inputs, weights, biases):
    V, D = pltpu.VMEM, pltpu.SemaphoreType.DMA
    rows, cols = inputs.shape[1], inputs.shape[2]
    n = CYCLES
    return pl.pallas_call(
        kernel,
        out_shape=jax.ShapeDtypeStruct((LAY,) + inputs.shape, F32),
        in_specs=[
            pl.BlockSpec(memory_space=pl.ANY),
            pl.BlockSpec(memory_space=pl.ANY),
            pl.BlockSpec(memory_space=pltpu.VMEM),
        ],
        out_specs=pl.BlockSpec(memory_space=pl.ANY),
        scratch_shapes=[
            V((rows, cols, CH), F32),
            V((H, TW, CH), F32),
            V((LAY, 9, CH, CH), F32),
            V((LAY, 9 * CH, 2 * CH), BF16),
            V((CH, CH), F32),
            V((2, PX + 2 * TW, 3 * CH), BF16),
            V((PX + 2 * LAY, CH), F32),
            V((PX, CH), F32),
            V((n, H, TW, CH), F32),
            V((n, H, TC, CH), F32),
            V((n, H, TC, CH), F32),
            V((n, Z, SH, CH), F32),
            V((n, Z, SH, CH), F32),
            V((n, H, TW, CH), F32),
            V((n, X, SH, CH), F32),
            V((n, SH, CH), F32),
            V((Z, CH, CH), F32),
            V((X, CH, CH), F32),
            V((CH, CH), F32),
            V((Z, CH, 2 * CH), BF16),
            V((CH, 2 * CH * (Z - 1)), BF16),
            V((Z * CH, 2 * CH), BF16),
            V((2 * CH, 2 * CH), BF16),
            V((LAY, H, TC, CH), F32),
            D((3,)), D((5,)), D((LAY,)), D((n, 3)), D((n, 3)), D((Z,)), D((Z,)), D((1,)), D((1,)),
            D((X,)), D((X,)), D((n, Z)), D((n, Z)), D((n, X)), D((n, X)), D((n, Z)), D((n, Z)),
            D((n, Z)), D((n, 2, H)), D((LAY,)), D((LAY,)), D((LAY,)), D((1,)),
        ],
        compiler_params=pltpu.CompilerParams(
            collective_id=0, has_side_effects=True, vmem_limit_bytes=48 * 1024 * 1024
        ),
    )(inputs, weights, biases)


def solution(mesh):
    return jax.shard_map(
        shards,
        mesh=mesh,
        in_specs=(P(None, "row", "col", None), P("layer", None, None, None), P("layer", None)),
        out_specs=P("layer", None, "row", "col", None),
        check_vma=False,
    )
```

```python
import jax
import jax.numpy as jnp
from jax import lax
from jax.experimental import pallas as pl
from jax.experimental.pallas import tpu as pltpu
from jax.sharding import PartitionSpec as P

MESH = pl.DeviceIdType.MESH
F32, BF16 = jnp.float32, jnp.bfloat16
CYCLES = 2
STEP = 0.2
X, Z = 4, 8
CH = 128
LAY = 8
H = 4
TC = 48
TW = TC + 2 * LAY
PX = H * TW
SH = H * TC // Z


def split(a):
    high = a.astype(BF16).astype(F32)
    return high, a - high


def paired(a):
    high, low = split(a)
    return jnp.concatenate([high, low], axis=1).astype(BF16)


def fold(r, m):
    return (r[:m, :CH] + r[:m, CH:]) + (r[m:, :CH] + r[m:, CH:])


def times(a, pair):
    high, low = split(a)
    stacked = jnp.concatenate([high, low], axis=0).astype(BF16)
    r = jnp.dot(stacked, pair, preferred_element_type=F32)
    return fold(r, a.shape[0])


def kernel(
    inp, wts, bias_in, out,
    xin, bias, x0, wf, wc, psum, a_buf, pad, mask, st, cc, rs, rz, bz, dp, tx, tb, pz, mx, mown, pc, qc, sc, nc, outb,
    s_in, r_in, w_sem, s_sh, r_sh, s_p, r_p, s_pf, r_pf, s_m, r_m, s_a, r_a, s_t, r_t, s_b, r_b,
    s_h, r_h, s_o, r_o, l_o, x_sem,
):
    sec = lax.axis_index("layer")
    r = lax.axis_index("row")
    c = lax.axis_index("col")
    ncol = lax.axis_size("col")
    x, z = sec // Z, sec % Z
    t = 2 * c + r
    last = 2 * ncol - 1

    def at(layer, row, col):
        return {"layer": layer, "row": row, "col": col}

    def remote(src, dst, ss, rr, dev):
        return pltpu.make_async_remote_copy(
            src_ref=src, dst_ref=dst, send_sem=ss, recv_sem=rr, device_id=dev, device_id_type=MESH
        )

    right_rc = (1 - r, c + r)
    left_rc = (1 - r, c - (1 - r))
    has_right, has_left = t < last, t > 0

    load_x = pltpu.make_async_copy(inp.at[0], xin, x_sem.at[0])
    load_x.start()
    load_b = pltpu.make_async_copy(bias_in, bias, x_sem.at[1])
    load_b.start()

    def load_w(l):
        return pltpu.make_async_copy(wts.at[l], wf.at[l], w_sem.at[l])

    for l in range(LAY):
        load_w(l).start()

    bar = pltpu.get_barrier_semaphore()

    def greet(dev):
        pl.semaphore_signal(bar, inc=1, device_id=dev, device_id_type=MESH)

    for k in range(1, Z):
        greet(at(x * Z + (z + k) % Z, r, c))
    for k in range(1, X):
        greet(at(((x + k) % X) * Z + z, r, c))

    up = (z == Z - 1) & (x < X - 1)
    down = (z == 0) & (x > 0)

    @pl.when(up)
    def _():
        greet(at(sec + 1, r, c))

    @pl.when(down)
    def _():
        greet(at(sec - 1, r, c))

    for ok, (rr, c2) in ((has_right, right_rc), (has_left, left_rc)):
        @pl.when(ok)
        def _():
            for k in range(Z):
                greet(at(x * Z + k, rr, c2))

            @pl.when(up)
            def _():
                greet(at(sec + 1, rr, c2))

            @pl.when(down)
            def _():
                greet(at(sec - 1, rr, c2))

    @pl.when(c < ncol - 1)
    def _():
        greet(at(sec, r, c + 1))

    @pl.when(c > 0)
    def _():
        greet(at(sec, r, c - 1))

    one = lambda cond: jnp.where(cond, 1, 0)
    sides = one(has_right) + one(has_left)
    peers = (Z - 1) + (X - 1) + sides * Z + (1 + sides) * (one(up) + one(down)) + one(c < ncol - 1) + one(c > 0)

    zero_cols = jnp.zeros((H, LAY, CH), F32)

    @pl.when(t == 0)
    def _():
        x0[:, 0:LAY, :] = zero_cols
        for i in range(CYCLES):
            st[i, :, 0:LAY, :] = zero_cols
            dp[i, :, 0:LAY, :] = zero_cols

    @pl.when(t == last)
    def _():
        x0[:, TW - LAY : TW, :] = zero_cols
        for i in range(CYCLES):
            st[i, :, TW - LAY : TW, :] = zero_cols
            dp[i, :, TW - LAY : TW, :] = zero_cols

    a_buf[...] = jnp.zeros_like(a_buf)
    pad[...] = jnp.zeros_like(pad)
    psum[...] = jnp.zeros_like(psum)
    column = lax.broadcasted_iota(jnp.int32, (H, TW, CH), 1)
    inside = ((column >= LAY) | (t > 0)) & ((column < TW - LAY) | (t < last))
    mask[...] = jnp.where(inside, 1.0, 0.0).astype(F32).reshape(PX, CH)

    def convert(l, carry):
        load_w(l).wait()
        total = psum[...]
        for k in range(9):
            w = wf[l, k]
            total = total + w
            wc[l, k * CH : (k + 1) * CH, :] = paired(w)
        psum[...] = total
        return carry

    lax.fori_loop(0, LAY, convert, 0)
    rows_i = lax.broadcasted_iota(jnp.int32, (CH, CH), 0)
    cols_i = lax.broadcasted_iota(jnp.int32, (CH, CH), 1)
    eye = jnp.where(rows_i == cols_i, 1.0, 0.0).astype(F32)
    psum[...] = eye + STEP * psum[...]
    load_x.wait()
    load_b.wait()
    pl.semaphore_wait(bar, peers)

    wide = TC + LAY
    half = pl.ds(2 * r, 2)
    mine = pl.ds(pl.multiple_of(LAY * (1 - r), LAY), wide)
    theirs = pl.ds(pl.multiple_of(LAY * r, LAY), wide)
    src_mine = pl.ds(pl.multiple_of((TC - LAY) * r, LAY), wide)
    src_theirs = pl.ds(pl.multiple_of((TC - LAY) * (1 - r), LAY), wide)
    to_core = remote(xin.at[:, src_theirs, :], x0.at[half, theirs, :], s_in.at[0], r_in.at[0], at(sec, 1 - r, c))
    to_right = remote(
        xin.at[:, pl.ds(2 * TC - LAY, LAY), :], x0.at[half, pl.ds(0, LAY), :], s_in.at[1], r_in.at[1 + r], at(sec, 0, c + 1)
    )
    to_left = remote(
        xin.at[:, pl.ds(0, LAY), :], x0.at[half, pl.ds(TW - LAY, LAY), :], s_in.at[2], r_in.at[3 + r], at(sec, 1, c - 1)
    )
    to_core.start()

    @pl.when(c < ncol - 1)
    def _():
        to_right.start()

    @pl.when(c > 0)
    def _():
        to_left.start()

    hrows = pl.ds(pl.multiple_of(r * (CH // 2), CH // 2), CH // 2)

    def p_copy(k):
        return remote(
            psum.at[hrows, :], pz.at[z, hrows, :], s_p.at[k], r_p.at[k], at(x * Z + (z + k) % Z, r, c)
        )

    for k in (4, 3, 5, 2, 6, 1, 7):
        p_copy(k).start()
    pz[z, hrows, :] = psum[hrows, :]
    x0[half, mine, :] = xin[:, src_mine, :]

    def got_in(i, cols):
        part = x0.at[pl.ds(0, 2), cols, :]
        return remote(part, part, s_in.at[0], r_in.at[i], at(sec, 1 - r, c))

    got_in(0, pl.ds(0, wide)).wait_recv()

    @pl.when((r == 0) & (c > 0))
    def _():
        got_in(1, pl.ds(0, LAY)).wait_recv()
        got_in(2, pl.ds(0, LAY)).wait_recv()

    @pl.when((r == 1) & (c < ncol - 1))
    def _():
        got_in(3, pl.ds(0, LAY)).wait_recv()
        got_in(4, pl.ds(0, LAY)).wait_recv()

    to_core.wait_send()

    @pl.when(c < ncol - 1)
    def _():
        to_right.wait_send()

    @pl.when(c > 0)
    def _():
        to_left.wait_send()

    def set_start(value):
        pad[LAY : LAY + PX, :] = value.reshape(PX, CH)

    def layer(l):
        v = pad[LAY : LAY + PX, :]
        for d in range(3):
            high, low = split(pad[LAY - 1 + d : LAY - 1 + d + PX, :])
            a_buf[0, TW : TW + PX, d * CH : (d + 1) * CH] = high.astype(BF16)
            a_buf[1, TW : TW + PX, d * CH : (d + 1) * CH] = low.astype(BF16)
        lhs = jnp.concatenate(
            [
                jnp.concatenate([a_buf[h, d * TW : d * TW + PX, :] for d in range(3)], axis=1)
                for h in range(2)
            ],
            axis=0,
        )
        pre = fold(jnp.dot(lhs, wc[l], preferred_element_type=F32), PX)
        new = (v + STEP * jnp.tanh(pre + bias[pl.ds(l, 1), :])) * mask[...]
        pad[LAY : LAY + PX, :] = new
        return new

    def core(value):
        return value.reshape(H, TW, CH)[:, LAY : LAY + TC, :]

    set_start(x0[...])

    def plain(l, carry):
        layer(l)
        return carry

    def shift(i):
        nxt = sec + 1
        main = remote(cc.at[i], st.at[i, :, pl.ds(LAY, TC), :], s_sh.at[i, 0], r_sh.at[i, 0], at(nxt, r, c))
        rgt = remote(
            cc.at[i, :, pl.ds(TC - LAY, LAY), :], st.at[i, :, pl.ds(0, LAY), :], s_sh.at[i, 1], r_sh.at[i, 1], at(nxt, *right_rc)
        )
        lft = remote(
            cc.at[i, :, pl.ds(0, LAY), :], st.at[i, :, pl.ds(TW - LAY, LAY), :], s_sh.at[i, 2], r_sh.at[i, 2], at(nxt, *left_rc)
        )
        return main, rgt, lft

    def shift_send(i):
        main, rgt, lft = shift(i)

        @pl.when(sec < X * Z - 1)
        def _():
            @pl.when(has_right)
            def _():
                rgt.start()

            @pl.when(has_left)
            def _():
                lft.start()

            main.start()

    def shift_wait(i):
        main, rgt, lft = shift(i)

        @pl.when(sec > 0)
        def _():
            main.wait_recv()

            @pl.when(has_left)
            def _():
                rgt.wait_recv()

            @pl.when(has_right)
            def _():
                lft.wait_recv()

        @pl.when(sec == 0)
        def _():
            st[i] = x0[...]

        @pl.when(sec < X * Z - 1)
        def _():
            main.wait_send()

            @pl.when(has_right)
            def _():
                rgt.wait_send()

            @pl.when(has_left)
            def _():
                lft.wait_send()

    def m_copy(k):
        return remote(mown, mx.at[x], s_m.at[k], r_m.at[k], at(((x + k) % X) * Z + z, r, c))

    def a_copy(i, k):
        j = (z + k) % Z
        part = rs.at[i, j // 2, pl.ds(pl.multiple_of(SH * (j % 2), LAY), SH), :]
        return remote(part, rz.at[i, z], s_a.at[i, k], r_a.at[i, k], at(x * Z + j, r, c))

    def t_copy(i, k):
        return remote(tb.at[i], tx.at[i, x], s_t.at[i, k], r_t.at[i, k], at(((x + k) % X) * Z + z, r, c))

    my_cols = pl.ds(pl.multiple_of(LAY + SH * (z % 2), LAY), SH)

    def b_copy(i, k):
        j = (z + k) % Z
        return remote(bz.at[i, j], dp.at[i, z // 2, my_cols, :], s_b.at[i, k], r_b.at[i, k], at(x * Z + j, r, c))

    def h_copy(i, k, side):
        frm = (SH - LAY) if side == 0 else 0
        to = 0 if side == 0 else TW - LAY
        rc = right_rc if side == 0 else left_rc
        return remote(
            bz.at[i, k, pl.ds(frm, LAY), :], dp.at[i, z // 2, pl.ds(to, LAY), :], s_h.at[i, k], r_h.at[i, side, z // 2],
            at(x * Z + k, *rc),
        )

    my_shard = (z // 2, pl.ds(pl.multiple_of(SH * (z % 2), LAY), SH))

    for i in range(CYCLES):
        lax.fori_loop(0, LAY, plain, 0)
        cc[i] = core(pad[LAY : LAY + PX, :])
        shift_send(i)
        if i == 0:
            for k in range(1, Z):
                p_copy(k).wait()
            forward = remote(pz.at[:, hrows, :], pz.at[:, hrows, :], s_pf.at[0], r_pf.at[0], at(sec, 1 - r, c))
            forward.start()
            forward.wait()
            prefix, suffix = pz[0], eye
            for k in range(Z):
                pc[k] = paired(pz[k])
            for k in range(Z):
                if k > 0:
                    prefix = times(prefix, pc[k])
                if k < Z - 1:
                    qc[:, 2 * CH * k : 2 * CH * (k + 1)] = paired(prefix)
                back = Z - 1 - k
                pair = paired(suffix)
                sc[back * CH : (back + 1) * CH, :] = pair
                if back > 0:
                    suffix = times(pz[back], pair)
            mown[...] = prefix
            for k in range(1, X):
                m_copy(k).start()
        shift_wait(i)
        set_start(st[i])
        lax.fori_loop(0, LAY, plain, 0)
        rs[i] = core(pad[LAY : LAY + PX, :]) - cc[i]
        for k in (4, 3, 5, 2, 6, 1, 7):
            a_copy(i, k).start()
        rz[i, z] = rs[i, my_shard[0], my_shard[1], :]
        if i == 0:
            for k in range(1, X):
                m_copy(k).wait()
            near = mx[jnp.maximum(x - 1, 0)]
            far = mx[jnp.maximum(x - 2, 0)]
            near = jnp.where(x >= 2, near, 0.0)
            far = jnp.where(x >= 3, far, 0.0)
            near_pair = paired(near)
            nc[0:CH, :] = near_pair
            nc[CH : 2 * CH, :] = paired(times(far, near_pair))
        for k in range(1, Z):
            a_copy(i, k).wait()
        joined = jnp.concatenate([rz[i, k] for k in range(Z)], axis=1)
        tb[i] = times(joined, sc[...])
        for k in range(1, X):
            t_copy(i, k).start()
        run = rz[i, 0]
        local = [run]
        for k in range(1, Z - 1):
            run = times(run, pc[k]) + rz[i, k]
            local.append(run)
        for k in range(1, X):
            t_copy(i, k).wait()
        before = [jnp.where(x >= d, tx[i, jnp.maximum(x - d, 0)], 0.0) for d in range(1, X)]
        carry = before[0] + times(jnp.concatenate(before[1:], axis=1), nc[...])
        bz[i, 0] = carry
        high, low = split(carry)
        spread = jnp.dot(jnp.concatenate([high, low], axis=0).astype(BF16), qc[...], preferred_element_type=F32)
        for k in range(1, Z):
            bz[i, k] = local[k - 1] + fold(spread[:, 2 * CH * (k - 1) : 2 * CH * k], SH)
        for k in (4, 3, 5, 2, 6, 1, 7):
            b_copy(i, k).start()

        @pl.when((z % 2 == 1) & has_right)
        def _():
            for k in range(Z):
                h_copy(i, k, 0).start()

        @pl.when((z % 2 == 0) & has_left)
        def _():
            for k in range(Z):
                h_copy(i, k, 1).start()

        dp[i, z // 2, my_cols, :] = bz[i, z]
        for k in range(1, Z):
            b_copy(i, k).wait()

        def halo_in(side, row):
            part = dp.at[i, row, pl.ds(0 if side == 0 else TW - LAY, LAY), :]
            return remote(part, part, s_h.at[i, 0], r_h.at[i, side, row], at(sec, 1 - r, c))

        @pl.when(has_left)
        def _():
            for row in range(H):
                halo_in(0, row).wait_recv()

        @pl.when(has_right)
        def _():
            for row in range(H):
                halo_in(1, row).wait_recv()

        @pl.when((z % 2 == 1) & has_right)
        def _():
            for k in range(Z):
                h_copy(i, k, 0).wait_send()

        @pl.when((z % 2 == 0) & has_left)
        def _():
            for k in range(Z):
                h_copy(i, k, 1).wait_send()

        set_start(st[i] + dp[i])

    out_cols = pl.ds(pl.multiple_of(TC * r, LAY), TC)

    def keep(l):
        return pltpu.make_async_copy(outb.at[l, half], out.at[l, 0, :, out_cols, :], l_o.at[l])

    def give(l):
        return remote(
            outb.at[l, pl.ds(2 * (1 - r), 2)], out.at[l, 0, :, out_cols, :], s_o.at[l], r_o.at[l], at(sec, 1 - r, c)
        )

    i = CYCLES - 1
    delta = times(dp[i, :, pl.ds(LAY, TC), :].reshape(H * TC, CH), paired(psum[...])).reshape(H, TC, CH) + rs[i]
    outb[LAY - 1] = cc[i] + delta
    keep(LAY - 1).start()
    give(LAY - 1).start()

    def final(l, carry):
        outb[l] = core(layer(l))
        keep(l).start()
        give(l).start()
        return carry

    lax.fori_loop(0, LAY - 1, final, 0)
    for l in range(LAY):
        keep(l).wait()
        give(l).wait()


def shards(inputs, weights, biases):
    V, D = pltpu.VMEM, pltpu.SemaphoreType.DMA
    rows, cols = inputs.shape[1], inputs.shape[2]
    n = CYCLES
    return pl.pallas_call(
        kernel,
        out_shape=jax.ShapeDtypeStruct((LAY,) + inputs.shape, F32),
        in_specs=[
            pl.BlockSpec(memory_space=pltpu.HBM),
            pl.BlockSpec(memory_space=pltpu.HBM),
            pl.BlockSpec(memory_space=pltpu.HBM),
        ],
        out_specs=pl.BlockSpec(memory_space=pl.ANY),
        scratch_shapes=[
            V((rows, cols, CH), F32),
            V((LAY, CH), F32),
            V((H, TW, CH), F32),
            V((LAY, 9, CH, CH), F32),
            V((LAY, 9 * CH, 2 * CH), BF16),
            V((CH, CH), F32),
            V((2, PX + 2 * TW, 3 * CH), BF16),
            V((PX + 2 * LAY, CH), F32),
            V((PX, CH), F32),
            V((n, H, TW, CH), F32),
            V((n, H, TC, CH), F32),
            V((n, H, TC, CH), F32),
            V((n, Z, SH, CH), F32),
            V((n, Z, SH, CH), F32),
            V((n, H, TW, CH), F32),
            V((n, X, SH, CH), F32),
            V((n, SH, CH), F32),
            V((Z, CH, CH), F32),
            V((X, CH, CH), F32),
            V((CH, CH), F32),
            V((Z, CH, 2 * CH), BF16),
            V((CH, 2 * CH * (Z - 1)), BF16),
            V((Z * CH, 2 * CH), BF16),
            V((2 * CH, 2 * CH), BF16),
            V((LAY, H, TC, CH), F32),
            D((3,)), D((5,)), D((LAY,)), D((n, 3)), D((n, 3)), D((Z,)), D((Z,)), D((1,)), D((1,)),
            D((X,)), D((X,)), D((n, Z)), D((n, Z)), D((n, X)), D((n, X)), D((n, Z)), D((n, Z)),
            D((n, Z)), D((n, 2, H)), D((LAY,)), D((LAY,)), D((LAY,)), D((2,)),
        ],
        compiler_params=pltpu.CompilerParams(
            collective_id=0, has_side_effects=True, vmem_limit_bytes=63000000
        ),
    )(inputs, weights, biases)


def solution(mesh):
    return jax.shard_map(
        shards,
        mesh=mesh,
        in_specs=(P(None, "row", "col", None), P("layer", None, None, None), P("layer", None)),
        out_specs=P("layer", None, "row", "col", None),
        check_vma=False,
    )
```

```python
import jax
import jax.numpy as jnp
from jax import lax
from jax.experimental import pallas as pl
from jax.experimental.pallas import tpu as pltpu
from jax.sharding import PartitionSpec as P

MESH = pl.DeviceIdType.MESH
F32, BF16 = jnp.float32, jnp.bfloat16
CYCLES = 2
STEP = 0.2
X, Z = 4, 8
CH = 128
LAY = 8
H = 4
TC = 48
TW = TC + 2 * LAY
PX = H * TW
SH = H * TC // Z


def split(a):
    high = a.astype(BF16).astype(F32)
    return high, a - high


def paired(a):
    high, low = split(a)
    return jnp.concatenate([high, low], axis=1).astype(BF16)


def fold(r, m):
    return (r[:m, :CH] + r[:m, CH:]) + (r[m:, :CH] + r[m:, CH:])


def times(a, pair):
    high, low = split(a)
    stacked = jnp.concatenate([high, low], axis=0).astype(BF16)
    r = jnp.dot(stacked, pair, preferred_element_type=F32)
    return fold(r, a.shape[0])


def kernel(
    inp, wts, bias_in, out,
    xin, bias, x0, wf, wc, psum, a_buf, pad, mask, st, cc, rs, rz, bz, dp, tx, tb, pz, mx, mown, pc, qc, sc, nc, outb,
    s_in, r_in, w_sem, s_sh, r_sh, s_p, r_p, s_pf, r_pf, s_m, r_m, s_a, r_a, s_t, r_t, s_b, r_b,
    s_h, r_h, s_o, r_o, l_o, x_sem, s_y, r_y, rounds,
):
    sec = lax.axis_index("layer")
    r = lax.axis_index("row")
    c = lax.axis_index("col")
    ncol = lax.axis_size("col")
    x, z = sec // Z, sec % Z
    t = 2 * c + r
    last = 2 * ncol - 1

    def at(layer, row, col):
        return {"layer": layer, "row": row, "col": col}

    def remote(src, dst, ss, rr, dev):
        return pltpu.make_async_remote_copy(
            src_ref=src, dst_ref=dst, send_sem=ss, recv_sem=rr, device_id=dev, device_id_type=MESH
        )

    right_rc = (1 - r, c + r)
    left_rc = (1 - r, c - (1 - r))
    has_right, has_left = t < last, t > 0

    load_x = pltpu.make_async_copy(inp.at[0], xin, x_sem.at[0])
    load_x.start()
    load_b = pltpu.make_async_copy(bias_in, bias, x_sem.at[1])
    load_b.start()

    def load_w(l):
        return pltpu.make_async_copy(wts.at[l], wf.at[l], w_sem.at[l])

    for l in range(LAY):
        load_w(l).start()

    bar = pltpu.get_barrier_semaphore()

    def greet(dev):
        pl.semaphore_signal(bar, inc=1, device_id=dev, device_id_type=MESH)

    up_rc, down_rc = at(sec, r, c + 1), at(sec, r, c - 1)
    around = [at(x * Z + (z + d) % Z, r, c) for d in (1, Z - 1)] + [at(((x + d) % X) * Z + z, r, c) for d in (1, X - 1)]
    for dev in around + [at(sec, 1 - r, c)]:
        greet(dev)
    has_next, has_prev = c < ncol - 1, c > 0

    @pl.when(has_next)
    def _():
        greet(up_rc)
        greet(at(sec, 1 - r, c + 1))

    @pl.when(has_prev)
    def _():
        greet(down_rc)
        greet(at(sec, 1 - r, c - 1))

    one = lambda cond: jnp.where(cond, 1, 0)
    sides = one(has_next) + one(has_prev)

    def tell(k):
        for dev in around:
            pl.semaphore_signal(rounds.at[k], inc=1, device_id=dev, device_id_type=MESH)

        @pl.when(has_next)
        def _():
            pl.semaphore_signal(rounds.at[k], inc=1, device_id=up_rc, device_id_type=MESH)

        @pl.when(has_prev)
        def _():
            pl.semaphore_signal(rounds.at[k], inc=1, device_id=down_rc, device_id_type=MESH)

    def hear(k):
        pl.semaphore_wait(rounds.at[k], len(around) + sides)

    zero_cols = jnp.zeros((H, LAY, CH), F32)

    @pl.when(t == 0)
    def _():
        x0[:, 0:LAY, :] = zero_cols
        for i in range(CYCLES):
            st[i, :, 0:LAY, :] = zero_cols
            dp[i, :, 0:LAY, :] = zero_cols

    @pl.when(t == last)
    def _():
        x0[:, TW - LAY : TW, :] = zero_cols
        for i in range(CYCLES):
            st[i, :, TW - LAY : TW, :] = zero_cols
            dp[i, :, TW - LAY : TW, :] = zero_cols

    a_buf[...] = jnp.zeros_like(a_buf)
    pad[...] = jnp.zeros_like(pad)
    psum[...] = jnp.zeros_like(psum)
    column = lax.broadcasted_iota(jnp.int32, (H, TW, CH), 1)
    inside = ((column >= LAY) | (t > 0)) & ((column < TW - LAY) | (t < last))
    mask[...] = jnp.where(inside, 1.0, 0.0).astype(F32).reshape(PX, CH)

    def convert(l, carry):
        load_w(l).wait()
        total = psum[...]
        for k in range(9):
            w = wf[l, k]
            total = total + w
            wc[l, k * CH : (k + 1) * CH, :] = paired(w)
        psum[...] = total
        return carry

    lax.fori_loop(0, 3, convert, 0)
    load_x.wait()
    load_b.wait()
    pl.semaphore_wait(bar, len(around) + 1 + 2 * sides)

    wide = TC + LAY
    half = pl.ds(2 * r, 2)
    mine = pl.ds(pl.multiple_of(LAY * (1 - r), LAY), wide)
    theirs = pl.ds(pl.multiple_of(LAY * r, LAY), wide)
    src_mine = pl.ds(pl.multiple_of((TC - LAY) * r, LAY), wide)
    src_theirs = pl.ds(pl.multiple_of((TC - LAY) * (1 - r), LAY), wide)
    to_core = remote(xin.at[:, src_theirs, :], x0.at[half, theirs, :], s_in.at[0], r_in.at[0], at(sec, 1 - r, c))
    to_right = remote(
        xin.at[:, pl.ds(2 * TC - LAY, LAY), :], x0.at[half, pl.ds(0, LAY), :], s_in.at[1], r_in.at[1 + r], at(sec, 0, c + 1)
    )
    to_left = remote(
        xin.at[:, pl.ds(0, LAY), :], x0.at[half, pl.ds(TW - LAY, LAY), :], s_in.at[2], r_in.at[3 + r], at(sec, 1, c - 1)
    )
    to_core.start()

    @pl.when(c < ncol - 1)
    def _():
        to_right.start()

    @pl.when(c > 0)
    def _():
        to_left.start()

    hrows = pl.ds(pl.multiple_of(r * (CH // 2), CH // 2), CH // 2)
    slab = CH // 8
    prows = pl.ds(pl.multiple_of(slab * (4 * r + c), slab), slab)

    def p_copy(k):
        return remote(
            psum.at[prows, :], pz.at[z, prows, :], s_p.at[k], r_p.at[k], at(x * Z + (z + k) % Z, r, c)
        )

    def y_copy(k):
        part = pz.at[:, prows, :]
        return remote(part, part, s_y.at[k], r_y.at[k], at(sec, r, (c + k) % 4))

    tell(0)
    x0[half, mine, :] = xin[:, src_mine, :]
    lax.fori_loop(3, 5, convert, 0)
    hear(0)
    tell(1)
    lax.fori_loop(5, LAY, convert, 0)
    rows_i = lax.broadcasted_iota(jnp.int32, (CH, CH), 0)
    cols_i = lax.broadcasted_iota(jnp.int32, (CH, CH), 1)
    eye = jnp.where(rows_i == cols_i, 1.0, 0.0).astype(F32)
    psum[...] = eye + STEP * psum[...]
    pz[z, prows, :] = psum[prows, :]
    hear(1)
    tell(2)

    def got_in(i, cols):
        part = x0.at[pl.ds(0, 2), cols, :]
        return remote(part, part, s_in.at[0], r_in.at[i], at(sec, 1 - r, c))

    got_in(0, pl.ds(0, wide)).wait_recv()

    @pl.when((r == 0) & (c > 0))
    def _():
        got_in(1, pl.ds(0, LAY)).wait_recv()
        got_in(2, pl.ds(0, LAY)).wait_recv()

    @pl.when((r == 1) & (c < ncol - 1))
    def _():
        got_in(3, pl.ds(0, LAY)).wait_recv()
        got_in(4, pl.ds(0, LAY)).wait_recv()

    to_core.wait_send()

    @pl.when(c < ncol - 1)
    def _():
        to_right.wait_send()

    @pl.when(c > 0)
    def _():
        to_left.wait_send()

    def set_start(value):
        pad[LAY : LAY + PX, :] = value.reshape(PX, CH)

    def layer(l):
        v = pad[LAY : LAY + PX, :]
        for d in range(3):
            high, low = split(pad[LAY - 1 + d : LAY - 1 + d + PX, :])
            a_buf[0, TW : TW + PX, d * CH : (d + 1) * CH] = high.astype(BF16)
            a_buf[1, TW : TW + PX, d * CH : (d + 1) * CH] = low.astype(BF16)
        def both(lo, hi, cols):
            return jnp.concatenate([a_buf[h, lo:hi, cols] for h in range(2)], axis=0)

        rows3 = PX - TW
        pair, third = slice(0, 2 * CH), slice(2 * CH, 3 * CH)
        mid = jnp.concatenate(
            [both(TW, TW + PX, pair), both(TW, TW + PX, third), both(0, PX, third)], axis=1
        )
        w_mid = jnp.concatenate([wc[l, 3 * CH : 6 * CH, :], wc[l, 2 * CH : 3 * CH, :]], axis=0)
        full = fold(jnp.dot(mid, w_mid, preferred_element_type=F32), PX)
        above = fold(jnp.dot(both(TW, PX, pair), wc[l, 0 : 2 * CH, :], preferred_element_type=F32), rows3)
        below = fold(
            jnp.dot(both(2 * TW, TW + PX, slice(0, 3 * CH)), wc[l, 6 * CH : 9 * CH, :], preferred_element_type=F32), rows3
        )
        blank = jnp.zeros((TW, CH), F32)
        pre = full + jnp.concatenate([blank, above], axis=0) + jnp.concatenate([below, blank], axis=0)
        new = (v + STEP * jnp.tanh(pre + bias[pl.ds(l, 1), :])) * mask[...]
        pad[LAY : LAY + PX, :] = new
        return new

    def core(value):
        return value.reshape(H, TW, CH)[:, LAY : LAY + TC, :]

    set_start(x0[...])

    def plain(l, carry):
        layer(l)
        return carry

    def shift(i):
        nxt = sec + 1
        main = remote(cc.at[i], st.at[i, :, pl.ds(LAY, TC), :], s_sh.at[i, 0], r_sh.at[i, 0], at(nxt, r, c))
        rgt = remote(
            cc.at[i, :, pl.ds(TC - LAY, LAY), :], st.at[i, :, pl.ds(0, LAY), :], s_sh.at[i, 1], r_sh.at[i, 1], at(nxt, *right_rc)
        )
        lft = remote(
            cc.at[i, :, pl.ds(0, LAY), :], st.at[i, :, pl.ds(TW - LAY, LAY), :], s_sh.at[i, 2], r_sh.at[i, 2], at(nxt, *left_rc)
        )
        return main, rgt, lft

    def shift_send(i):
        main, rgt, lft = shift(i)

        @pl.when(sec < X * Z - 1)
        def _():
            @pl.when(has_right)
            def _():
                rgt.start()

            @pl.when(has_left)
            def _():
                lft.start()

            main.start()

    def shift_wait(i):
        main, rgt, lft = shift(i)

        @pl.when(sec > 0)
        def _():
            main.wait_recv()

            @pl.when(has_left)
            def _():
                rgt.wait_recv()

            @pl.when(has_right)
            def _():
                lft.wait_recv()

        @pl.when(sec == 0)
        def _():
            st[i] = x0[...]

        @pl.when(sec < X * Z - 1)
        def _():
            main.wait_send()

            @pl.when(has_right)
            def _():
                rgt.wait_send()

            @pl.when(has_left)
            def _():
                lft.wait_send()

    def m_copy(k):
        return remote(mown, mx.at[x], s_m.at[k], r_m.at[k], at(((x + k) % X) * Z + z, r, c))

    def a_copy(i, k):
        j = (z + k) % Z
        part = rs.at[i, j // 2, pl.ds(pl.multiple_of(SH * (j % 2), LAY), SH), :]
        return remote(part, rz.at[i, z], s_a.at[i, k], r_a.at[i, k], at(x * Z + j, r, c))

    def t_copy(i, k):
        return remote(tb.at[i], tx.at[i, x], s_t.at[i, k], r_t.at[i, k], at(((x + k) % X) * Z + z, r, c))

    my_cols = pl.ds(pl.multiple_of(LAY + SH * (z % 2), LAY), SH)

    def b_copy(i, k):
        j = (z + k) % Z
        return remote(bz.at[i, j], dp.at[i, z // 2, my_cols, :], s_b.at[i, k], r_b.at[i, k], at(x * Z + j, r, c))

    def h_copy(i, k, side):
        frm = (SH - LAY) if side == 0 else 0
        to = 0 if side == 0 else TW - LAY
        rc = right_rc if side == 0 else left_rc
        return remote(
            bz.at[i, k, pl.ds(frm, LAY), :], dp.at[i, z // 2, pl.ds(to, LAY), :], s_h.at[i, k], r_h.at[i, side, z // 2],
            at(x * Z + k, *rc),
        )

    my_shard = (z // 2, pl.ds(pl.multiple_of(SH * (z % 2), LAY), SH))

    for i in range(CYCLES):
        if i == 0:
            lax.fori_loop(0, 2, plain, 0)
            hear(2)
            tell(3)
            lax.fori_loop(2, 4, plain, 0)
            hear(3)
            for k in (4, 3, 5, 2, 6, 1, 7):
                p_copy(k).start()
            lax.fori_loop(4, LAY, plain, 0)
        else:
            lax.fori_loop(0, LAY, plain, 0)
        cc[i] = core(pad[LAY : LAY + PX, :])
        shift_send(i)
        if i == 0:
            for k in range(1, Z):
                p_copy(k).wait()
            for k in (2, 1, 3):
                y_copy(k).start()
        shift_wait(i)
        set_start(st[i])
        lax.fori_loop(0, LAY, plain, 0)
        rs[i] = core(pad[LAY : LAY + PX, :]) - cc[i]
        for k in (4, 3, 5, 2, 6, 1, 7):
            a_copy(i, k).start()
        rz[i, z] = rs[i, my_shard[0], my_shard[1], :]
        if i == 0:
            for k in range(1, 4):
                y_copy(k).wait()
            forward = remote(pz.at[:, hrows, :], pz.at[:, hrows, :], s_pf.at[0], r_pf.at[0], at(sec, 1 - r, c))
            forward.start()
            forward.wait()
            prefix, suffix = pz[0], eye
            for k in range(Z):
                pc[k] = paired(pz[k])
            for k in range(Z):
                if k > 0:
                    prefix = times(prefix, pc[k])
                if k < Z - 1:
                    qc[:, 2 * CH * k : 2 * CH * (k + 1)] = paired(prefix)
                back = Z - 1 - k
                pair = paired(suffix)
                sc[back * CH : (back + 1) * CH, :] = pair
                if back > 0:
                    suffix = times(pz[back], pair)
            mown[...] = prefix
            for k in range(1, X):
                m_copy(k).start()
        for k in range(1, Z):
            a_copy(i, k).wait()
        joined = jnp.concatenate([rz[i, k] for k in range(Z)], axis=1)
        tb[i] = times(joined, sc[...])
        for k in range(1, X):
            t_copy(i, k).start()
        run = rz[i, 0]
        local = [run]
        for k in range(1, Z - 1):
            run = times(run, pc[k]) + rz[i, k]
            local.append(run)
        if i == 0:
            for k in range(1, X):
                m_copy(k).wait()
            near = mx[jnp.maximum(x - 1, 0)]
            far = mx[jnp.maximum(x - 2, 0)]
            near = jnp.where(x >= 2, near, 0.0)
            far = jnp.where(x >= 3, far, 0.0)
            near_pair = paired(near)
            nc[0:CH, :] = near_pair
            nc[CH : 2 * CH, :] = paired(times(far, near_pair))
        for k in range(1, X):
            t_copy(i, k).wait()
        before = [jnp.where(x >= d, tx[i, jnp.maximum(x - d, 0)], 0.0) for d in range(1, X)]
        carry = before[0] + times(jnp.concatenate(before[1:], axis=1), nc[...])
        bz[i, 0] = carry
        high, low = split(carry)
        spread = jnp.dot(jnp.concatenate([high, low], axis=0).astype(BF16), qc[...], preferred_element_type=F32)
        for k in range(1, Z):
            bz[i, k] = local[k - 1] + fold(spread[:, 2 * CH * (k - 1) : 2 * CH * k], SH)
        for k in (4, 3, 5, 2, 6, 1, 7):
            b_copy(i, k).start()

        @pl.when((z % 2 == 1) & has_right)
        def _():
            for k in range(Z):
                h_copy(i, k, 0).start()

        @pl.when((z % 2 == 0) & has_left)
        def _():
            for k in range(Z):
                h_copy(i, k, 1).start()

        dp[i, z // 2, my_cols, :] = bz[i, z]
        for k in range(1, Z):
            b_copy(i, k).wait()

        def halo_in(side, row):
            part = dp.at[i, row, pl.ds(0 if side == 0 else TW - LAY, LAY), :]
            return remote(part, part, s_h.at[i, 0], r_h.at[i, side, row], at(sec, 1 - r, c))

        if i == CYCLES - 1:
            before = dp[i, :, pl.ds(LAY, TC), :].reshape(H * TC, CH)
            delta = times(before, paired(psum[...])).reshape(H, TC, CH) + rs[i]
            outb[LAY - 1] = cc[i] + delta

        @pl.when(has_left)
        def _():
            for row in range(H):
                halo_in(0, row).wait_recv()

        @pl.when(has_right)
        def _():
            for row in range(H):
                halo_in(1, row).wait_recv()

        @pl.when((z % 2 == 1) & has_right)
        def _():
            for k in range(Z):
                h_copy(i, k, 0).wait_send()

        @pl.when((z % 2 == 0) & has_left)
        def _():
            for k in range(Z):
                h_copy(i, k, 1).wait_send()

        set_start(st[i] + dp[i])

    out_cols = pl.ds(pl.multiple_of(TC * r, LAY), TC)

    def keep(l):
        return pltpu.make_async_copy(outb.at[l, half], out.at[l, 0, :, out_cols, :], l_o.at[l])

    def give(l):
        return remote(
            outb.at[l, pl.ds(2 * (1 - r), 2)], out.at[l, 0, :, out_cols, :], s_o.at[l], r_o.at[l], at(sec, 1 - r, c)
        )

    keep(LAY - 1).start()
    give(LAY - 1).start()

    def final(l, carry):
        outb[l] = core(layer(l))
        keep(l).start()
        give(l).start()
        return carry

    lax.fori_loop(0, LAY - 1, final, 0)
    for l in range(LAY):
        keep(l).wait()
        give(l).wait()


def shards(inputs, weights, biases):
    V, D = pltpu.VMEM, pltpu.SemaphoreType.DMA
    rows, cols = inputs.shape[1], inputs.shape[2]
    n = CYCLES
    return pl.pallas_call(
        kernel,
        out_shape=jax.ShapeDtypeStruct((LAY,) + inputs.shape, F32),
        in_specs=[
            pl.BlockSpec(memory_space=pltpu.HBM),
            pl.BlockSpec(memory_space=pltpu.HBM),
            pl.BlockSpec(memory_space=pltpu.HBM),
        ],
        out_specs=pl.BlockSpec(memory_space=pl.ANY),
        scratch_shapes=[
            V((rows, cols, CH), F32),
            V((LAY, CH), F32),
            V((H, TW, CH), F32),
            V((LAY, 9, CH, CH), F32),
            V((LAY, 9 * CH, 2 * CH), BF16),
            V((CH, CH), F32),
            V((2, PX + 2 * TW, 3 * CH), BF16),
            V((PX + 2 * LAY, CH), F32),
            V((PX, CH), F32),
            V((n, H, TW, CH), F32),
            V((n, H, TC, CH), F32),
            V((n, H, TC, CH), F32),
            V((n, Z, SH, CH), F32),
            V((n, Z, SH, CH), F32),
            V((n, H, TW, CH), F32),
            V((n, X, SH, CH), F32),
            V((n, SH, CH), F32),
            V((Z, CH, CH), F32),
            V((X, CH, CH), F32),
            V((CH, CH), F32),
            V((Z, CH, 2 * CH), BF16),
            V((CH, 2 * CH * (Z - 1)), BF16),
            V((Z * CH, 2 * CH), BF16),
            V((2 * CH, 2 * CH), BF16),
            V((LAY, H, TC, CH), F32),
            D((3,)), D((5,)), D((LAY,)), D((n, 3)), D((n, 3)), D((Z,)), D((Z,)), D((1,)), D((1,)),
            D((X,)), D((X,)), D((n, Z)), D((n, Z)), D((n, X)), D((n, X)), D((n, Z)), D((n, Z)),
            D((n, Z)), D((n, 2, H)), D((LAY,)), D((LAY,)), D((LAY,)), D((2,)),
            D((4,)), D((4,)), pltpu.SemaphoreType.REGULAR((4,)),
        ],
        compiler_params=pltpu.CompilerParams(
            collective_id=0, has_side_effects=True, vmem_limit_bytes=63000000
        ),
    )(inputs, weights, biases)


def solution(mesh):
    return jax.shard_map(
        shards,
        mesh=mesh,
        in_specs=(P(None, "row", "col", None), P("layer", None, None, None), P("layer", None)),
        out_specs=P("layer", None, "row", "col", None),
        check_vma=False,
    )
```

```python
import jax
import jax.numpy as jnp
from jax import lax
from jax.experimental import pallas as pl
from jax.experimental.pallas import tpu as pltpu
from jax.sharding import PartitionSpec as P

MESH = pl.DeviceIdType.MESH
F32, BF16 = jnp.float32, jnp.bfloat16
CYCLES = 2
STEP = 0.2
X, Z = 4, 8
CH = 128
LAY = 8
H = 4
TC = 48
TW = TC + 2 * LAY
PX = H * TW
SH = H * TC // Z


def split(a):
    high = a.astype(BF16).astype(F32)
    return high, a - high


def paired(a):
    high, low = split(a)
    return jnp.concatenate([high, low], axis=1).astype(BF16)


def fold(r, m):
    return (r[:m, :CH] + r[:m, CH:]) + (r[m:, :CH] + r[m:, CH:])


def times(a, pair):
    high, low = split(a)
    stacked = jnp.concatenate([high, low], axis=0).astype(BF16)
    r = jnp.dot(stacked, pair, preferred_element_type=F32)
    return fold(r, a.shape[0])


def kernel(
    inp, wts, bias_in, out,
    xin, bias, x0, wf, wc, wp, beside, psum, a_buf, pad, mask, st, cc, rs, rz, bz, dp, tx, tb, pz, mx, mown, pc, qc, sc, nc, outb,
    s_in, r_in, w_sem, s_sh, r_sh, s_p, r_p, s_pf, r_pf, s_m, r_m, s_a, r_a, s_t, r_t, s_b, r_b,
    s_h, r_h, s_o, r_o, l_o, x_sem, s_y, r_y, rounds,
):
    sec = lax.axis_index("layer")
    r = lax.axis_index("row")
    c = lax.axis_index("col")
    ncol = lax.axis_size("col")
    x, z = sec // Z, sec % Z
    t = 2 * c + r
    last = 2 * ncol - 1

    def at(layer, row, col):
        return {"layer": layer, "row": row, "col": col}

    def remote(src, dst, ss, rr, dev):
        return pltpu.make_async_remote_copy(
            src_ref=src, dst_ref=dst, send_sem=ss, recv_sem=rr, device_id=dev, device_id_type=MESH
        )

    right_rc = (1 - r, c + r)
    left_rc = (1 - r, c - (1 - r))
    has_right, has_left = t < last, t > 0

    load_x = pltpu.make_async_copy(inp.at[0], xin, x_sem.at[0])
    load_x.start()
    load_b = pltpu.make_async_copy(bias_in, bias, x_sem.at[1])
    load_b.start()

    def load_w(l):
        return pltpu.make_async_copy(wts.at[l], wf.at[l], w_sem.at[l])

    for l in range(LAY):
        load_w(l).start()

    bar = pltpu.get_barrier_semaphore()

    def greet(dev):
        pl.semaphore_signal(bar, inc=1, device_id=dev, device_id_type=MESH)

    up_rc, down_rc = at(sec, r, c + 1), at(sec, r, c - 1)
    around = [at(x * Z + (z + d) % Z, r, c) for d in (1, Z - 1)] + [at(((x + d) % X) * Z + z, r, c) for d in (1, X - 1)]
    for dev in around + [at(sec, 1 - r, c)]:
        greet(dev)
    has_next, has_prev = c < ncol - 1, c > 0

    @pl.when(has_next)
    def _():
        greet(up_rc)
        greet(at(sec, 1 - r, c + 1))

    @pl.when(has_prev)
    def _():
        greet(down_rc)
        greet(at(sec, 1 - r, c - 1))

    one = lambda cond: jnp.where(cond, 1, 0)
    sides = one(has_next) + one(has_prev)

    def tell(k):
        for dev in around:
            pl.semaphore_signal(rounds.at[k], inc=1, device_id=dev, device_id_type=MESH)

        @pl.when(has_next)
        def _():
            pl.semaphore_signal(rounds.at[k], inc=1, device_id=up_rc, device_id_type=MESH)

        @pl.when(has_prev)
        def _():
            pl.semaphore_signal(rounds.at[k], inc=1, device_id=down_rc, device_id_type=MESH)

    def hear(k):
        pl.semaphore_wait(rounds.at[k], len(around) + sides)

    zero_cols = jnp.zeros((H, LAY, CH), F32)

    @pl.when(t == 0)
    def _():
        x0[:, 0:LAY, :] = zero_cols
        for i in range(CYCLES):
            st[i, :, 0:LAY, :] = zero_cols
            dp[i, :, 0:LAY, :] = zero_cols

    @pl.when(t == last)
    def _():
        x0[:, TW - LAY : TW, :] = zero_cols
        for i in range(CYCLES):
            st[i, :, TW - LAY : TW, :] = zero_cols
            dp[i, :, TW - LAY : TW, :] = zero_cols

    a_buf[...] = jnp.zeros_like(a_buf)
    beside[...] = jnp.zeros_like(beside)
    pad[...] = jnp.zeros_like(pad)
    psum[...] = jnp.zeros_like(psum)
    column = lax.broadcasted_iota(jnp.int32, (H, TW, CH), 1)
    inside = ((column >= LAY) | (t > 0)) & ((column < TW - LAY) | (t < last))
    mask[...] = jnp.where(inside, 1.0, 0.0).astype(F32).reshape(PX, CH)

    def convert(l, carry):
        load_w(l).wait()
        total = psum[...]
        for k in range(9):
            w = wf[l, k]
            total = total + w
            duo = paired(w)
            wc[l, k * CH : (k + 1) * CH, :] = duo
            row, left = ((k % 3, k < 3), (3 + min(k % 3, 1), k < 5))[k // 3 == 1]
            wp[l, row * CH : (row + 1) * CH, (0 if left else CH) : (CH if left else 2 * CH)] = duo[:, :CH]
        wp[l, 3 * CH : 4 * CH, CH:] = jnp.zeros((CH, CH), BF16)
        psum[...] = total
        return carry

    load_x.wait()
    load_b.wait()
    pl.semaphore_wait(bar, len(around) + 1 + 2 * sides)

    wide = TC + LAY
    half = pl.ds(2 * r, 2)
    mine = pl.ds(pl.multiple_of(LAY * (1 - r), LAY), wide)
    theirs = pl.ds(pl.multiple_of(LAY * r, LAY), wide)
    src_mine = pl.ds(pl.multiple_of((TC - LAY) * r, LAY), wide)
    src_theirs = pl.ds(pl.multiple_of((TC - LAY) * (1 - r), LAY), wide)
    to_core = remote(xin.at[:, src_theirs, :], x0.at[half, theirs, :], s_in.at[0], r_in.at[0], at(sec, 1 - r, c))
    to_right = remote(
        xin.at[:, pl.ds(2 * TC - LAY, LAY), :], x0.at[half, pl.ds(0, LAY), :], s_in.at[1], r_in.at[1 + r], at(sec, 0, c + 1)
    )
    to_left = remote(
        xin.at[:, pl.ds(0, LAY), :], x0.at[half, pl.ds(TW - LAY, LAY), :], s_in.at[2], r_in.at[3 + r], at(sec, 1, c - 1)
    )
    to_core.start()

    @pl.when(c < ncol - 1)
    def _():
        to_right.start()

    @pl.when(c > 0)
    def _():
        to_left.start()

    hrows = pl.ds(pl.multiple_of(r * (CH // 2), CH // 2), CH // 2)
    slab = CH // 8
    prows = pl.ds(pl.multiple_of(slab * (4 * r + c), slab), slab)

    def p_copy(k):
        return remote(
            psum.at[prows, :], pz.at[z, prows, :], s_p.at[k], r_p.at[k], at(x * Z + (z + k) % Z, r, c)
        )

    def y_copy(k):
        part = pz.at[:, prows, :]
        return remote(part, part, s_y.at[k], r_y.at[k], at(sec, r, (c + k) % 4))

    tell(0)
    x0[half, mine, :] = xin[:, src_mine, :]
    lax.fori_loop(0, 4, convert, 0)
    hear(0)
    tell(1)
    lax.fori_loop(4, LAY, convert, 0)
    rows_i = lax.broadcasted_iota(jnp.int32, (CH, CH), 0)
    cols_i = lax.broadcasted_iota(jnp.int32, (CH, CH), 1)
    eye = jnp.where(rows_i == cols_i, 1.0, 0.0).astype(F32)
    psum[...] = eye + STEP * psum[...]
    pz[z, prows, :] = psum[prows, :]
    hear(1)
    tell(2)

    def got_in(i, cols):
        part = x0.at[pl.ds(0, 2), cols, :]
        return remote(part, part, s_in.at[0], r_in.at[i], at(sec, 1 - r, c))

    got_in(0, pl.ds(0, wide)).wait_recv()

    @pl.when((r == 0) & (c > 0))
    def _():
        got_in(1, pl.ds(0, LAY)).wait_recv()
        got_in(2, pl.ds(0, LAY)).wait_recv()

    @pl.when((r == 1) & (c < ncol - 1))
    def _():
        got_in(3, pl.ds(0, LAY)).wait_recv()
        got_in(4, pl.ds(0, LAY)).wait_recv()

    to_core.wait_send()

    @pl.when(c < ncol - 1)
    def _():
        to_right.wait_send()

    @pl.when(c > 0)
    def _():
        to_left.wait_send()

    def set_start(value):
        pad[LAY : LAY + PX, :] = value.reshape(PX, CH)

    def layer(l):
        v = pad[LAY : LAY + PX, :]
        for d in range(3):
            high, low = split(pad[LAY - 1 + d : LAY - 1 + d + PX, :])
            a_buf[0, TW : TW + PX, d * CH : (d + 1) * CH] = high.astype(BF16)
            a_buf[1, TW : TW + PX, d * CH : (d + 1) * CH] = low.astype(BF16)
        rows3 = PX - TW
        pair, third = slice(0, 2 * CH), slice(2 * CH, 3 * CH)
        image, upper = slice(TW, TW + PX), slice(0, PX)

        def dot(a, b):
            return jnp.dot(a, b, preferred_element_type=F32)

        def flat(r):
            return r[:, :CH] + r[:, CH:]

        low_rows = dot(a_buf[1, image, :], wp[l, 0 : 3 * CH, :])
        low_mid = dot(a_buf[1, image, pair], wp[l, 3 * CH : 5 * CH, :])
        beside[0:PX, :] = low_mid[:, CH:]
        mid = jnp.concatenate([a_buf[0, image, pair], a_buf[0, image, third], a_buf[0, upper, third]], axis=1)
        w_mid = jnp.concatenate([wc[l, 3 * CH : 6 * CH, :], wc[l, 2 * CH : 3 * CH, :]], axis=0)
        full = flat(dot(mid, w_mid)) + low_mid[:, :CH] + beside[1 : PX + 1, :]
        above = flat(dot(a_buf[0, TW:PX, pair], wc[l, 0 : 2 * CH, :])) + low_rows[:rows3, :CH]
        below = flat(dot(a_buf[0, 2 * TW : TW + PX, :], wc[l, 6 * CH : 9 * CH, :])) + low_rows[TW:, CH:]
        blank = jnp.zeros((TW, CH), F32)
        pre = full + jnp.concatenate([blank, above], axis=0) + jnp.concatenate([below, blank], axis=0)
        new = (v + STEP * jnp.tanh(pre + bias[pl.ds(l, 1), :])) * mask[...]
        pad[LAY : LAY + PX, :] = new
        return new

    def core(value):
        return value.reshape(H, TW, CH)[:, LAY : LAY + TC, :]

    set_start(x0[...])

    def plain(l, carry):
        layer(l)
        return carry

    def shift(i):
        nxt = sec + 1
        main = remote(cc.at[i], st.at[i, :, pl.ds(LAY, TC), :], s_sh.at[i, 0], r_sh.at[i, 0], at(nxt, r, c))
        rgt = remote(
            cc.at[i, :, pl.ds(TC - LAY, LAY), :], st.at[i, :, pl.ds(0, LAY), :], s_sh.at[i, 1], r_sh.at[i, 1], at(nxt, *right_rc)
        )
        lft = remote(
            cc.at[i, :, pl.ds(0, LAY), :], st.at[i, :, pl.ds(TW - LAY, LAY), :], s_sh.at[i, 2], r_sh.at[i, 2], at(nxt, *left_rc)
        )
        return main, rgt, lft

    def shift_send(i):
        main, rgt, lft = shift(i)

        @pl.when(sec < X * Z - 1)
        def _():
            @pl.when(has_right)
            def _():
                rgt.start()

            @pl.when(has_left)
            def _():
                lft.start()

            main.start()

    def shift_wait(i):
        main, rgt, lft = shift(i)

        @pl.when(sec > 0)
        def _():
            main.wait_recv()

            @pl.when(has_left)
            def _():
                rgt.wait_recv()

            @pl.when(has_right)
            def _():
                lft.wait_recv()

        @pl.when(sec == 0)
        def _():
            st[i] = x0[...]

        @pl.when(sec < X * Z - 1)
        def _():
            main.wait_send()

            @pl.when(has_right)
            def _():
                rgt.wait_send()

            @pl.when(has_left)
            def _():
                lft.wait_send()

    def m_copy(k):
        return remote(mown, mx.at[x], s_m.at[k], r_m.at[k], at(((x + k) % X) * Z + z, r, c))

    def a_copy(i, k):
        j = (z + k) % Z
        part = rs.at[i, j // 2, pl.ds(pl.multiple_of(SH * (j % 2), LAY), SH), :]
        return remote(part, rz.at[i, z], s_a.at[i, k], r_a.at[i, k], at(x * Z + j, r, c))

    def t_copy(i, k):
        return remote(tb.at[i], tx.at[i, x], s_t.at[i, k], r_t.at[i, k], at(((x + k) % X) * Z + z, r, c))

    my_cols = pl.ds(pl.multiple_of(LAY + SH * (z % 2), LAY), SH)

    def b_copy(i, k):
        j = (z + k) % Z
        return remote(bz.at[i, j], dp.at[i, z // 2, my_cols, :], s_b.at[i, k], r_b.at[i, k], at(x * Z + j, r, c))

    def h_copy(i, k, side):
        frm = (SH - LAY) if side == 0 else 0
        to = 0 if side == 0 else TW - LAY
        rc = right_rc if side == 0 else left_rc
        return remote(
            bz.at[i, (z + k) % Z, pl.ds(frm, LAY), :], dp.at[i, z // 2, pl.ds(to, LAY), :], s_h.at[i, k], r_h.at[i, side, z // 2],
            at(x * Z + (z + k) % Z, *rc),
        )

    my_shard = (z // 2, pl.ds(pl.multiple_of(SH * (z % 2), LAY), SH))

    for i in range(CYCLES):
        if i == 0:
            lax.fori_loop(0, 2, plain, 0)
            hear(2)
            tell(3)
            for k in (4, 3, 5, 2, 6, 1, 7):
                p_copy(k).start()
            lax.fori_loop(2, LAY, plain, 0)
            hear(3)
        else:
            lax.fori_loop(0, LAY, plain, 0)
        cc[i] = core(pad[LAY : LAY + PX, :])
        shift_send(i)
        if i == 0:
            for k in range(1, Z):
                p_copy(k).wait()
            for k in (2, 1, 3):
                y_copy(k).start()
        shift_wait(i)
        set_start(st[i])
        lax.fori_loop(0, LAY, plain, 0)
        rs[i] = core(pad[LAY : LAY + PX, :]) - cc[i]
        for k in (4, 3, 5, 2, 6, 1, 7):
            a_copy(i, k).start()
        rz[i, z] = rs[i, my_shard[0], my_shard[1], :]
        if i == 0:
            for k in range(1, 4):
                y_copy(k).wait()
            forward = remote(pz.at[:, hrows, :], pz.at[:, hrows, :], s_pf.at[0], r_pf.at[0], at(sec, 1 - r, c))
            forward.start()
            forward.wait()
            prefix, suffix = pz[0], eye
            for k in range(Z):
                pc[k] = paired(pz[k])
            for k in range(Z):
                if k > 0:
                    prefix = times(prefix, pc[k])
                if k < Z - 1:
                    qc[:, 2 * CH * k : 2 * CH * (k + 1)] = paired(prefix)
                back = Z - 1 - k
                pair = paired(suffix)
                sc[back * CH : (back + 1) * CH, :] = pair
                if back > 0:
                    suffix = times(pz[back], pair)
            mown[...] = prefix
            for k in range(1, X):
                m_copy(k).start()
        for k in range(1, Z):
            a_copy(i, k).wait()
        joined = jnp.concatenate([rz[i, k] for k in range(Z)], axis=1)
        tb[i] = times(joined, sc[...])
        for k in range(1, X):
            t_copy(i, k).start()
        run = rz[i, 0]
        local = [run]
        for k in range(1, Z - 1):
            run = times(run, pc[k]) + rz[i, k]
            local.append(run)
        if i == 0:
            for k in range(1, X):
                m_copy(k).wait()
            near = mx[jnp.maximum(x - 1, 0)]
            far = mx[jnp.maximum(x - 2, 0)]
            near = jnp.where(x >= 2, near, 0.0)
            far = jnp.where(x >= 3, far, 0.0)
            near_pair = paired(near)
            nc[0:CH, :] = near_pair
            nc[CH : 2 * CH, :] = paired(times(far, near_pair))
        for k in range(1, X):
            t_copy(i, k).wait()
        before = [jnp.where(x >= d, tx[i, jnp.maximum(x - d, 0)], 0.0) for d in range(1, X)]
        carry = before[0] + times(jnp.concatenate(before[1:], axis=1), nc[...])
        bz[i, 0] = carry
        high, low = split(carry)
        spread = jnp.dot(jnp.concatenate([high, low], axis=0).astype(BF16), qc[...], preferred_element_type=F32)
        for k in range(1, Z):
            bz[i, k] = local[k - 1] + fold(spread[:, 2 * CH * (k - 1) : 2 * CH * k], SH)
        @pl.when((z % 2 == 1) & has_right)
        def _():
            for k in (4, 3, 5, 2, 6, 1, 7, 0):
                h_copy(i, k, 0).start()

        @pl.when((z % 2 == 0) & has_left)
        def _():
            for k in (4, 3, 5, 2, 6, 1, 7, 0):
                h_copy(i, k, 1).start()

        for k in (4, 3, 5, 2, 6, 1, 7):
            b_copy(i, k).start()

        dp[i, z // 2, my_cols, :] = bz[i, z]
        for k in range(1, Z):
            b_copy(i, k).wait()

        def halo_in(side, row):
            part = dp.at[i, row, pl.ds(0 if side == 0 else TW - LAY, LAY), :]
            return remote(part, part, s_h.at[i, 0], r_h.at[i, side, row], at(sec, 1 - r, c))

        if i == CYCLES - 1:
            before = dp[i, :, pl.ds(LAY, TC), :].reshape(H * TC, CH)
            delta = times(before, paired(psum[...])).reshape(H, TC, CH) + rs[i]
            outb[LAY - 1] = cc[i] + delta

        @pl.when(has_left)
        def _():
            for row in range(H):
                halo_in(0, row).wait_recv()

        @pl.when(has_right)
        def _():
            for row in range(H):
                halo_in(1, row).wait_recv()

        @pl.when((z % 2 == 1) & has_right)
        def _():
            for k in range(Z):
                h_copy(i, k, 0).wait_send()

        @pl.when((z % 2 == 0) & has_left)
        def _():
            for k in range(Z):
                h_copy(i, k, 1).wait_send()

        set_start(st[i] + dp[i])

    out_cols = pl.ds(pl.multiple_of(TC * r, LAY), TC)

    def keep(l):
        return pltpu.make_async_copy(outb.at[l, half], out.at[l, 0, :, out_cols, :], l_o.at[l])

    def give(l):
        return remote(
            outb.at[l, pl.ds(2 * (1 - r), 2)], out.at[l, 0, :, out_cols, :], s_o.at[l], r_o.at[l], at(sec, 1 - r, c)
        )

    keep(LAY - 1).start()
    give(LAY - 1).start()

    def final(l, carry):
        outb[l] = core(layer(l))
        keep(l).start()
        give(l).start()
        return carry

    lax.fori_loop(0, LAY - 1, final, 0)
    for l in range(LAY):
        keep(l).wait()
        give(l).wait()


def shards(inputs, weights, biases):
    V, D = pltpu.VMEM, pltpu.SemaphoreType.DMA
    rows, cols = inputs.shape[1], inputs.shape[2]
    n = CYCLES
    return pl.pallas_call(
        kernel,
        out_shape=jax.ShapeDtypeStruct((LAY,) + inputs.shape, F32),
        in_specs=[
            pl.BlockSpec(memory_space=pltpu.HBM),
            pl.BlockSpec(memory_space=pltpu.HBM),
            pl.BlockSpec(memory_space=pltpu.HBM),
        ],
        out_specs=pl.BlockSpec(memory_space=pl.ANY),
        scratch_shapes=[
            V((rows, cols, CH), F32),
            V((LAY, CH), F32),
            V((H, TW, CH), F32),
            V((LAY, 9, CH, CH), F32),
            V((LAY, 9 * CH, 2 * CH), BF16),
            V((LAY, 5 * CH, 2 * CH), BF16),
            V((PX + LAY, CH), F32),
            V((CH, CH), F32),
            V((2, PX + 2 * TW, 3 * CH), BF16),
            V((PX + 2 * LAY, CH), F32),
            V((PX, CH), F32),
            V((n, H, TW, CH), F32),
            V((n, H, TC, CH), F32),
            V((n, H, TC, CH), F32),
            V((n, Z, SH, CH), F32),
            V((n, Z, SH, CH), F32),
            V((n, H, TW, CH), F32),
            V((n, X, SH, CH), F32),
            V((n, SH, CH), F32),
            V((Z, CH, CH), F32),
            V((X, CH, CH), F32),
            V((CH, CH), F32),
            V((Z, CH, 2 * CH), BF16),
            V((CH, 2 * CH * (Z - 1)), BF16),
            V((Z * CH, 2 * CH), BF16),
            V((2 * CH, 2 * CH), BF16),
            V((LAY, H, TC, CH), F32),
            D((3,)), D((5,)), D((LAY,)), D((n, 3)), D((n, 3)), D((Z,)), D((Z,)), D((1,)), D((1,)),
            D((X,)), D((X,)), D((n, Z)), D((n, Z)), D((n, X)), D((n, X)), D((n, Z)), D((n, Z)),
            D((n, Z)), D((n, 2, H)), D((LAY,)), D((LAY,)), D((LAY,)), D((2,)),
            D((4,)), D((4,)), pltpu.SemaphoreType.REGULAR((4,)),
        ],
        compiler_params=pltpu.CompilerParams(
            collective_id=0, has_side_effects=True, vmem_limit_bytes=54000000
        ),
    )(pltpu.with_memory_space_constraint(inputs, pltpu.HBM), weights, pltpu.with_memory_space_constraint(biases, pltpu.HBM))


def solution(mesh):
    return jax.shard_map(
        shards,
        mesh=mesh,
        in_specs=(P(None, "row", "col", None), P("layer", None, None, None), P("layer", None)),
        out_specs=P("layer", None, "row", "col", None),
        check_vma=False,
    )
```

```python
import jax
import jax.numpy as jnp
from jax import lax
from jax.experimental import pallas as pl
from jax.experimental.pallas import tpu as pltpu
from jax.sharding import PartitionSpec as P

MESH = pl.DeviceIdType.MESH
F32, BF16 = jnp.float32, jnp.bfloat16
CYCLES = 2
STEP = 0.2
X, Z = 4, 8
CH = 128
LAY = 8
H = 4
TC = 48
TW = TC + 2 * LAY
PX = H * TW
SH = H * TC // Z


def split(a):
    high = a.astype(BF16).astype(F32)
    return high, a - high


def paired(a):
    high, low = split(a)
    return jnp.concatenate([high, low], axis=1).astype(BF16)


def fold(r, m):
    return (r[:m, :CH] + r[:m, CH:]) + (r[m:, :CH] + r[m:, CH:])


def times(a, pair):
    high, low = split(a)
    stacked = jnp.concatenate([high, low], axis=0).astype(BF16)
    r = jnp.dot(stacked, pair, preferred_element_type=F32)
    return fold(r, a.shape[0])


def kernel(
    inp, wts, bias_in, out,
    xin, bias, x0, wf, wc, wp, beside, psum, a_buf, pad, mask, st, cc, rs, rz, bz, dp, tx, tb, pz, mx, mown, pc, qc, sc, nc, outb,
    s_in, r_in, w_sem, s_sh, r_sh, s_p, r_p, s_pf, r_pf, s_m, r_m, s_a, r_a, s_t, r_t, s_b, r_b,
    s_h, r_h, s_o, r_o, l_o, x_sem, s_y, r_y, rounds,
):
    sec = lax.axis_index("layer")
    r = lax.axis_index("row")
    c = lax.axis_index("col")
    ncol = lax.axis_size("col")
    x, z = sec // Z, sec % Z
    t = 2 * c + r
    last = 2 * ncol - 1

    def at(layer, row, col):
        return {"layer": layer, "row": row, "col": col}

    def remote(src, dst, ss, rr, dev):
        return pltpu.make_async_remote_copy(
            src_ref=src, dst_ref=dst, send_sem=ss, recv_sem=rr, device_id=dev, device_id_type=MESH
        )

    right_rc = (1 - r, c + r)
    left_rc = (1 - r, c - (1 - r))
    has_right, has_left = t < last, t > 0

    load_x = pltpu.make_async_copy(inp.at[0], xin, x_sem.at[0])
    load_x.start()
    load_b = pltpu.make_async_copy(bias_in, bias, x_sem.at[1])
    load_b.start()

    def load_w(l):
        return pltpu.make_async_copy(wts.at[l], wf.at[l], w_sem.at[l])

    for l in range(LAY):
        load_w(l).start()

    bar = pltpu.get_barrier_semaphore()

    def greet(dev):
        pl.semaphore_signal(bar, inc=1, device_id=dev, device_id_type=MESH)

    up_rc, down_rc = at(sec, r, c + 1), at(sec, r, c - 1)
    around = [at(x * Z + (z + d) % Z, r, c) for d in (1, Z - 1)] + [at(((x + d) % X) * Z + z, r, c) for d in (1, X - 1)]
    for dev in around + [at(sec, 1 - r, c)]:
        greet(dev)
    has_next, has_prev = c < ncol - 1, c > 0

    @pl.when(has_next)
    def _():
        greet(up_rc)
        greet(at(sec, 1 - r, c + 1))

    @pl.when(has_prev)
    def _():
        greet(down_rc)
        greet(at(sec, 1 - r, c - 1))

    one = lambda cond: jnp.where(cond, 1, 0)
    sides = one(has_next) + one(has_prev)

    def tell(k):
        for dev in around:
            pl.semaphore_signal(rounds.at[k], inc=1, device_id=dev, device_id_type=MESH)

        @pl.when(has_next)
        def _():
            pl.semaphore_signal(rounds.at[k], inc=1, device_id=up_rc, device_id_type=MESH)

        @pl.when(has_prev)
        def _():
            pl.semaphore_signal(rounds.at[k], inc=1, device_id=down_rc, device_id_type=MESH)

    def hear(k):
        pl.semaphore_wait(rounds.at[k], len(around) + sides)

    zero_cols = jnp.zeros((H, LAY, CH), F32)

    @pl.when(t == 0)
    def _():
        x0[:, 0:LAY, :] = zero_cols
        for i in range(CYCLES):
            st[i, :, 0:LAY, :] = zero_cols
            dp[i, :, 0:LAY, :] = zero_cols

    @pl.when(t == last)
    def _():
        x0[:, TW - LAY : TW, :] = zero_cols
        for i in range(CYCLES):
            st[i, :, TW - LAY : TW, :] = zero_cols
            dp[i, :, TW - LAY : TW, :] = zero_cols

    a_buf[...] = jnp.zeros_like(a_buf)
    beside[...] = jnp.zeros_like(beside)
    pad[...] = jnp.zeros_like(pad)
    psum[...] = jnp.zeros_like(psum)
    column = lax.broadcasted_iota(jnp.int32, (H, TW, CH), 1)
    inside = ((column >= LAY) | (t > 0)) & ((column < TW - LAY) | (t < last))
    mask[...] = jnp.where(inside, 1.0, 0.0).astype(F32).reshape(PX, CH)

    def convert(l, carry):
        load_w(l).wait()
        total = psum[...]
        for k in range(9):
            w = wf[l, k]
            total = total + w
            duo = paired(w)
            wc[l, k * CH : (k + 1) * CH, :] = duo
            row, left = ((k % 3, k < 3), (3 + min(k % 3, 1), k < 5))[k // 3 == 1]
            wp[l, row * CH : (row + 1) * CH, (0 if left else CH) : (CH if left else 2 * CH)] = duo[:, :CH]
        wp[l, 3 * CH : 4 * CH, CH:] = jnp.zeros((CH, CH), BF16)
        psum[...] = total
        return carry

    load_x.wait()
    load_b.wait()
    pl.semaphore_wait(bar, len(around) + 1 + 2 * sides)

    wide = TC + LAY
    half = pl.ds(2 * r, 2)
    mine = pl.ds(pl.multiple_of(LAY * (1 - r), LAY), wide)
    theirs = pl.ds(pl.multiple_of(LAY * r, LAY), wide)
    src_mine = pl.ds(pl.multiple_of((TC - LAY) * r, LAY), wide)
    src_theirs = pl.ds(pl.multiple_of((TC - LAY) * (1 - r), LAY), wide)
    to_core = remote(xin.at[:, src_theirs, :], x0.at[half, theirs, :], s_in.at[0], r_in.at[0], at(sec, 1 - r, c))
    to_right = remote(
        xin.at[:, pl.ds(2 * TC - LAY, LAY), :], x0.at[half, pl.ds(0, LAY), :], s_in.at[1], r_in.at[1 + r], at(sec, 0, c + 1)
    )
    to_left = remote(
        xin.at[:, pl.ds(0, LAY), :], x0.at[half, pl.ds(TW - LAY, LAY), :], s_in.at[2], r_in.at[3 + r], at(sec, 1, c - 1)
    )
    to_core.start()

    @pl.when(c < ncol - 1)
    def _():
        to_right.start()

    @pl.when(c > 0)
    def _():
        to_left.start()

    hrows = pl.ds(pl.multiple_of(r * (CH // 2), CH // 2), CH // 2)
    slab = CH // 8
    prows = pl.ds(pl.multiple_of(slab * (4 * r + c), slab), slab)

    def p_copy(k):
        return remote(
            psum.at[prows, :], pz.at[z, prows, :], s_p.at[k], r_p.at[k], at(x * Z + (z + k) % Z, r, c)
        )

    def y_copy(k):
        part = pz.at[:, prows, :]
        return remote(part, part, s_y.at[k], r_y.at[k], at(sec, r, (c + k) % 4))

    tell(0)
    x0[half, mine, :] = xin[:, src_mine, :]
    lax.fori_loop(0, 4, convert, 0)
    hear(0)
    tell(1)
    lax.fori_loop(4, LAY, convert, 0)
    rows_i = lax.broadcasted_iota(jnp.int32, (CH, CH), 0)
    cols_i = lax.broadcasted_iota(jnp.int32, (CH, CH), 1)
    eye = jnp.where(rows_i == cols_i, 1.0, 0.0).astype(F32)
    psum[...] = eye + STEP * psum[...]
    pz[z, prows, :] = psum[prows, :]
    hear(1)
    tell(2)

    def got_in(i, cols):
        part = x0.at[pl.ds(0, 2), cols, :]
        return remote(part, part, s_in.at[0], r_in.at[i], at(sec, 1 - r, c))

    got_in(0, pl.ds(0, wide)).wait_recv()

    @pl.when((r == 0) & (c > 0))
    def _():
        got_in(1, pl.ds(0, LAY)).wait_recv()
        got_in(2, pl.ds(0, LAY)).wait_recv()

    @pl.when((r == 1) & (c < ncol - 1))
    def _():
        got_in(3, pl.ds(0, LAY)).wait_recv()
        got_in(4, pl.ds(0, LAY)).wait_recv()

    to_core.wait_send()

    @pl.when(c < ncol - 1)
    def _():
        to_right.wait_send()

    @pl.when(c > 0)
    def _():
        to_left.wait_send()

    def set_start(value):
        pad[LAY : LAY + PX, :] = value.reshape(PX, CH)

    def layer(l):
        v = pad[LAY : LAY + PX, :]
        for d in range(3):
            high, low = split(pad[LAY - 1 + d : LAY - 1 + d + PX, :])
            a_buf[0, TW : TW + PX, d * CH : (d + 1) * CH] = high.astype(BF16)
            a_buf[1, TW : TW + PX, d * CH : (d + 1) * CH] = low.astype(BF16)
        rows3 = PX - TW
        pair, third = slice(0, 2 * CH), slice(2 * CH, 3 * CH)
        image, upper = slice(TW, TW + PX), slice(0, PX)

        def dot(a, b):
            return jnp.dot(a, b, preferred_element_type=F32)

        def flat(r):
            return r[:, :CH] + r[:, CH:]

        low_rows = dot(a_buf[1, image, :], wp[l, 0 : 3 * CH, :])
        low_mid = dot(a_buf[1, image, pair], wp[l, 3 * CH : 5 * CH, :])
        beside[0:PX, :] = low_mid[:, CH:]
        mid = jnp.concatenate([a_buf[0, image, pair], a_buf[0, image, third], a_buf[0, upper, third]], axis=1)
        w_mid = jnp.concatenate([wc[l, 3 * CH : 6 * CH, :], wc[l, 2 * CH : 3 * CH, :]], axis=0)
        full = flat(dot(mid, w_mid)) + low_mid[:, :CH] + beside[1 : PX + 1, :]
        above = flat(dot(a_buf[0, TW:PX, pair], wc[l, 0 : 2 * CH, :])) + low_rows[:rows3, :CH]
        below = flat(dot(a_buf[0, 2 * TW : TW + PX, :], wc[l, 6 * CH : 9 * CH, :])) + low_rows[TW:, CH:]
        blank = jnp.zeros((TW, CH), F32)
        pre = full + jnp.concatenate([blank, above], axis=0) + jnp.concatenate([below, blank], axis=0)
        new = (v + STEP * jnp.tanh(pre + bias[pl.ds(l, 1), :])) * mask[...]
        pad[LAY : LAY + PX, :] = new
        return new

    def core(value):
        return value.reshape(H, TW, CH)[:, LAY : LAY + TC, :]

    set_start(x0[...])

    def plain(l, carry):
        layer(l)
        return carry

    def shift(i):
        nxt = sec + 1
        main = remote(cc.at[i], st.at[i, :, pl.ds(LAY, TC), :], s_sh.at[i, 0], r_sh.at[i, 0], at(nxt, r, c))
        rgt = remote(
            cc.at[i, :, pl.ds(TC - LAY, LAY), :], st.at[i, :, pl.ds(0, LAY), :], s_sh.at[i, 1], r_sh.at[i, 1], at(nxt, *right_rc)
        )
        lft = remote(
            cc.at[i, :, pl.ds(0, LAY), :], st.at[i, :, pl.ds(TW - LAY, LAY), :], s_sh.at[i, 2], r_sh.at[i, 2], at(nxt, *left_rc)
        )
        return main, rgt, lft

    def shift_send(i):
        main, rgt, lft = shift(i)

        @pl.when(sec < X * Z - 1)
        def _():
            @pl.when(has_right)
            def _():
                rgt.start()

            @pl.when(has_left)
            def _():
                lft.start()

            main.start()

    def shift_wait(i):
        main, rgt, lft = shift(i)

        @pl.when(sec > 0)
        def _():
            main.wait_recv()

            @pl.when(has_left)
            def _():
                rgt.wait_recv()

            @pl.when(has_right)
            def _():
                lft.wait_recv()

        @pl.when(sec == 0)
        def _():
            st[i] = x0[...]

        @pl.when(sec < X * Z - 1)
        def _():
            main.wait_send()

            @pl.when(has_right)
            def _():
                rgt.wait_send()

            @pl.when(has_left)
            def _():
                lft.wait_send()

    def m_copy(k):
        return remote(mown, mx.at[x], s_m.at[k], r_m.at[k], at(((x + k) % X) * Z + z, r, c))

    def a_copy(i, k):
        j = (z + k) % Z
        part = rs.at[i, j // 2, pl.ds(pl.multiple_of(SH * (j % 2), LAY), SH), :]
        return remote(part, rz.at[i, z], s_a.at[i, k], r_a.at[i, k], at(x * Z + j, 1 - r, c))

    def t_copy(i, k):
        return remote(tb.at[i], tx.at[i, x], s_t.at[i, k], r_t.at[i, k], at(((x + k) % X) * Z + z, r, c))

    my_cols = pl.ds(pl.multiple_of(LAY + SH * (z % 2), LAY), SH)

    def b_copy(i, k):
        j = (z + k) % Z
        return remote(bz.at[i, j], dp.at[i, z // 2, my_cols, :], s_b.at[i, k], r_b.at[i, k], at(x * Z + j, 1 - r, c))

    def h_copy(i, k, side):
        frm = (SH - LAY) if side == 0 else 0
        to = 0 if side == 0 else TW - LAY
        rc = (r, c + 1 - r) if side == 0 else (r, c - r)
        return remote(
            bz.at[i, (z + k) % Z, pl.ds(frm, LAY), :], dp.at[i, z // 2, pl.ds(to, LAY), :], s_h.at[i, k], r_h.at[i, side, z // 2],
            at(x * Z + (z + k) % Z, *rc),
        )

    odd = z % 2 == 1
    own_right, own_left = odd & (2 * c + 1 - r < last), (z % 2 == 0) & (2 * c + 1 - r > 0)
    inner_right, inner_left = odd & (r == 1), (z % 2 == 0) & (r == 0)

    for i in range(CYCLES):
        if i == 0:
            lax.fori_loop(0, 2, plain, 0)
            hear(2)
            tell(3)
            for k in (4, 3, 5, 2, 6, 1, 7):
                p_copy(k).start()
            lax.fori_loop(2, LAY, plain, 0)
            hear(3)
        else:
            lax.fori_loop(0, LAY, plain, 0)
        cc[i] = core(pad[LAY : LAY + PX, :])
        shift_send(i)
        if i == 0:
            for k in range(1, Z):
                p_copy(k).wait()
            for k in (2, 1, 3):
                y_copy(k).start()
        shift_wait(i)
        set_start(st[i])
        lax.fori_loop(0, LAY, plain, 0)
        rs[i] = core(pad[LAY : LAY + PX, :]) - cc[i]
        for k in (4, 3, 5, 2, 6, 1, 7, 0):
            a_copy(i, k).start()
        if i == 0:
            for k in range(1, 4):
                y_copy(k).wait()
            forward = remote(pz.at[:, hrows, :], pz.at[:, hrows, :], s_pf.at[0], r_pf.at[0], at(sec, 1 - r, c))
            forward.start()
            forward.wait()
            prefix, suffix = pz[0], eye
            for k in range(Z):
                pc[k] = paired(pz[k])
            for k in range(Z):
                if k > 0:
                    prefix = times(prefix, pc[k])
                if k < Z - 1:
                    qc[:, 2 * CH * k : 2 * CH * (k + 1)] = paired(prefix)
                back = Z - 1 - k
                pair = paired(suffix)
                sc[back * CH : (back + 1) * CH, :] = pair
                if back > 0:
                    suffix = times(pz[back], pair)
            mown[...] = prefix
            for k in range(1, X):
                m_copy(k).start()
        for k in range(Z):
            a_copy(i, k).wait()
        joined = jnp.concatenate([rz[i, k] for k in range(Z)], axis=1)
        tb[i] = times(joined, sc[...])
        for k in range(1, X):
            t_copy(i, k).start()
        run = rz[i, 0]
        local = [run]
        for k in range(1, Z - 1):
            run = times(run, pc[k]) + rz[i, k]
            local.append(run)
        if i == 0:
            for k in range(1, X):
                m_copy(k).wait()
            near = mx[jnp.maximum(x - 1, 0)]
            far = mx[jnp.maximum(x - 2, 0)]
            near = jnp.where(x >= 2, near, 0.0)
            far = jnp.where(x >= 3, far, 0.0)
            near_pair = paired(near)
            nc[0:CH, :] = near_pair
            nc[CH : 2 * CH, :] = paired(times(far, near_pair))
        for k in range(1, X):
            t_copy(i, k).wait()
        before = [jnp.where(x >= d, tx[i, jnp.maximum(x - d, 0)], 0.0) for d in range(1, X)]
        carry = before[0] + times(jnp.concatenate(before[1:], axis=1), nc[...])
        bz[i, 0] = carry
        high, low = split(carry)
        spread = jnp.dot(jnp.concatenate([high, low], axis=0).astype(BF16), qc[...], preferred_element_type=F32)
        for k in range(1, Z):
            bz[i, k] = local[k - 1] + fold(spread[:, 2 * CH * (k - 1) : 2 * CH * k], SH)
        for side, sends, inner in ((0, own_right, inner_right), (1, own_left, inner_left)):
            @pl.when(sends)
            def _():
                for k in (4, 3, 5, 2, 6, 1, 7):
                    h_copy(i, k, side).start()

                @pl.when(jnp.logical_not(inner))
                def _():
                    h_copy(i, 0, side).start()

        for k in (4, 3, 5, 2, 6, 1, 7, 0):
            b_copy(i, k).start()

        @pl.when(inner_right)
        def _():
            dp[i, z // 2, 0:LAY, :] = bz[i, z, SH - LAY : SH, :]

        @pl.when(inner_left)
        def _():
            dp[i, z // 2, TW - LAY : TW, :] = bz[i, z, 0:LAY, :]

        for k in range(Z):
            b_copy(i, k).wait()

        def halo_in(side, row):
            part = dp.at[i, row, pl.ds(0 if side == 0 else TW - LAY, LAY), :]
            return remote(part, part, s_h.at[i, 0], r_h.at[i, side, row], at(sec, 1 - r, c))

        if i == CYCLES - 1:
            before = dp[i, :, pl.ds(LAY, TC), :].reshape(H * TC, CH)
            delta = times(before, paired(psum[...])).reshape(H, TC, CH) + rs[i]
            outb[LAY - 1] = cc[i] + delta

        for side, comes, inner in ((0, has_left, inner_right), (1, has_right, inner_left)):
            @pl.when(comes)
            def _():
                for row in range(H):
                    @pl.when(jnp.logical_not(inner & (z // 2 == row)))
                    def _():
                        halo_in(side, row).wait_recv()

        for side, sends, inner in ((0, own_right, inner_right), (1, own_left, inner_left)):
            @pl.when(sends)
            def _():
                for k in range(1, Z):
                    h_copy(i, k, side).wait_send()

                @pl.when(jnp.logical_not(inner))
                def _():
                    h_copy(i, 0, side).wait_send()

        set_start(st[i] + dp[i])

    out_cols = pl.ds(pl.multiple_of(TC * r, LAY), TC)

    def keep(l):
        return pltpu.make_async_copy(outb.at[l, half], out.at[l, 0, :, out_cols, :], l_o.at[l])

    def give(l):
        return remote(
            outb.at[l, pl.ds(2 * (1 - r), 2)], out.at[l, 0, :, out_cols, :], s_o.at[l], r_o.at[l], at(sec, 1 - r, c)
        )

    keep(LAY - 1).start()
    give(LAY - 1).start()

    def final(l, carry):
        outb[l] = core(layer(l))
        keep(l).start()
        give(l).start()
        return carry

    lax.fori_loop(0, LAY - 1, final, 0)
    for l in range(LAY):
        keep(l).wait()
        give(l).wait()


def shards(inputs, weights, biases):
    V, D = pltpu.VMEM, pltpu.SemaphoreType.DMA
    rows, cols = inputs.shape[1], inputs.shape[2]
    n = CYCLES
    return pl.pallas_call(
        kernel,
        out_shape=jax.ShapeDtypeStruct((LAY,) + inputs.shape, F32),
        in_specs=[
            pl.BlockSpec(memory_space=pltpu.HBM),
            pl.BlockSpec(memory_space=pltpu.HBM),
            pl.BlockSpec(memory_space=pltpu.HBM),
        ],
        out_specs=pl.BlockSpec(memory_space=pl.ANY),
        scratch_shapes=[
            V((rows, cols, CH), F32),
            V((LAY, CH), F32),
            V((H, TW, CH), F32),
            V((LAY, 9, CH, CH), F32),
            V((LAY, 9 * CH, 2 * CH), BF16),
            V((LAY, 5 * CH, 2 * CH), BF16),
            V((PX + LAY, CH), F32),
            V((CH, CH), F32),
            V((2, PX + 2 * TW, 3 * CH), BF16),
            V((PX + 2 * LAY, CH), F32),
            V((PX, CH), F32),
            V((n, H, TW, CH), F32),
            V((n, H, TC, CH), F32),
            V((n, H, TC, CH), F32),
            V((n, Z, SH, CH), F32),
            V((n, Z, SH, CH), F32),
            V((n, H, TW, CH), F32),
            V((n, X, SH, CH), F32),
            V((n, SH, CH), F32),
            V((Z, CH, CH), F32),
            V((X, CH, CH), F32),
            V((CH, CH), F32),
            V((Z, CH, 2 * CH), BF16),
            V((CH, 2 * CH * (Z - 1)), BF16),
            V((Z * CH, 2 * CH), BF16),
            V((2 * CH, 2 * CH), BF16),
            V((LAY, H, TC, CH), F32),
            D((3,)), D((5,)), D((LAY,)), D((n, 3)), D((n, 3)), D((Z,)), D((Z,)), D((1,)), D((1,)),
            D((X,)), D((X,)), D((n, Z)), D((n, Z)), D((n, X)), D((n, X)), D((n, Z)), D((n, Z)),
            D((n, Z)), D((n, 2, H)), D((LAY,)), D((LAY,)), D((LAY,)), D((2,)),
            D((4,)), D((4,)), pltpu.SemaphoreType.REGULAR((4,)),
        ],
        compiler_params=pltpu.CompilerParams(
            collective_id=0, has_side_effects=True, vmem_limit_bytes=54000000
        ),
    )(pltpu.with_memory_space_constraint(inputs, pltpu.HBM), weights, pltpu.with_memory_space_constraint(biases, pltpu.HBM))


def solution(mesh):
    return jax.shard_map(
        shards,
        mesh=mesh,
        in_specs=(P(None, "row", "col", None), P("layer", None, None, None), P("layer", None)),
        out_specs=P("layer", None, "row", "col", None),
        check_vma=False,
    )
```

```python
import jax
import jax.numpy as jnp
from jax import lax
from jax.experimental import pallas as pl
from jax.experimental.pallas import tpu as pltpu
from jax.sharding import PartitionSpec as P

MESH = pl.DeviceIdType.MESH
F32, BF16 = jnp.float32, jnp.bfloat16
CYCLES = 2
STEP = 0.2
X, Z = 4, 8
CH = 128
LAY = 8
H = 4
TC = 48
TW = TC + 2 * LAY
PX = H * TW
SH = H * TC // Z


def split(a):
    high = a.astype(BF16).astype(F32)
    return high, a - high


def paired(a):
    high, low = split(a)
    return jnp.concatenate([high, low], axis=1).astype(BF16)


def fold(r, m):
    return (r[:m, :CH] + r[:m, CH:]) + (r[m:, :CH] + r[m:, CH:])


def times(a, pair):
    high, low = split(a)
    stacked = jnp.concatenate([high, low], axis=0).astype(BF16)
    r = jnp.dot(stacked, pair, preferred_element_type=F32)
    return fold(r, a.shape[0])


def kernel(
    inp, wts, bias_in, out,
    xin, bias, x0, wf, wc, wp, beside, psum, a_buf, pad, mask, st, cc, rs, rz, bz, dp, tx, tb, pz, mx, mown, pc, qc, sc, nc, outb,
    s_in, r_in, w_sem, s_sh, r_sh, s_p, r_p, s_pf, r_pf, s_m, r_m, s_a, r_a, s_t, r_t, s_b, r_b,
    s_h, r_h, s_o, r_o, l_o, x_sem, s_y, r_y, rounds,
):
    sec = lax.axis_index("layer")
    r = lax.axis_index("row")
    c = lax.axis_index("col")
    ncol = lax.axis_size("col")
    x, z = sec // Z, sec % Z
    t = 2 * c + r
    last = 2 * ncol - 1

    def at(layer, row, col):
        return {"layer": layer, "row": row, "col": col}

    def remote(src, dst, ss, rr, dev):
        return pltpu.make_async_remote_copy(
            src_ref=src, dst_ref=dst, send_sem=ss, recv_sem=rr, device_id=dev, device_id_type=MESH
        )

    right_rc = (1 - r, c + r)
    left_rc = (1 - r, c - (1 - r))
    has_right, has_left = t < last, t > 0

    load_x = pltpu.make_async_copy(inp.at[0], xin, x_sem.at[0])
    load_x.start()
    load_b = pltpu.make_async_copy(bias_in, bias, x_sem.at[1])
    load_b.start()

    def load_w(l):
        return pltpu.make_async_copy(wts.at[l], wf.at[l], w_sem.at[l])

    for l in range(LAY):
        load_w(l).start()

    bar = pltpu.get_barrier_semaphore()

    def greet(dev):
        pl.semaphore_signal(bar, inc=1, device_id=dev, device_id_type=MESH)

    up_rc, down_rc = at(sec, r, c + 1), at(sec, r, c - 1)
    around = [at(x * Z + (z + d) % Z, r, c) for d in (1, Z - 1)] + [at(((x + d) % X) * Z + z, r, c) for d in (1, X - 1)]
    for dev in around + [at(sec, 1 - r, c)]:
        greet(dev)
    has_next, has_prev = c < ncol - 1, c > 0

    @pl.when(has_next)
    def _():
        greet(up_rc)
        greet(at(sec, 1 - r, c + 1))

    @pl.when(has_prev)
    def _():
        greet(down_rc)
        greet(at(sec, 1 - r, c - 1))

    one = lambda cond: jnp.where(cond, 1, 0)
    sides = one(has_next) + one(has_prev)

    def tell(k):
        for dev in around:
            pl.semaphore_signal(rounds.at[k], inc=1, device_id=dev, device_id_type=MESH)

        @pl.when(has_next)
        def _():
            pl.semaphore_signal(rounds.at[k], inc=1, device_id=up_rc, device_id_type=MESH)

        @pl.when(has_prev)
        def _():
            pl.semaphore_signal(rounds.at[k], inc=1, device_id=down_rc, device_id_type=MESH)

    def hear(k):
        pl.semaphore_wait(rounds.at[k], len(around) + sides)

    zero_cols = jnp.zeros((H, LAY, CH), F32)

    @pl.when(t == 0)
    def _():
        x0[:, 0:LAY, :] = zero_cols
        for i in range(CYCLES):
            st[i, :, 0:LAY, :] = zero_cols
            dp[i, :, 0:LAY, :] = zero_cols

    @pl.when(t == last)
    def _():
        x0[:, TW - LAY : TW, :] = zero_cols
        for i in range(CYCLES):
            st[i, :, TW - LAY : TW, :] = zero_cols
            dp[i, :, TW - LAY : TW, :] = zero_cols

    a_buf[...] = jnp.zeros_like(a_buf)
    beside[...] = jnp.zeros_like(beside)
    pad[...] = jnp.zeros_like(pad)
    psum[...] = jnp.zeros_like(psum)
    column = lax.broadcasted_iota(jnp.int32, (H, TW, CH), 1)
    inside = ((column >= LAY) | (t > 0)) & ((column < TW - LAY) | (t < last))
    mask[...] = jnp.where(inside, 1.0, 0.0).astype(F32).reshape(PX, CH)

    def convert(l, carry):
        load_w(l).wait()
        total = psum[...]
        for k in range(9):
            w = wf[l, k]
            total = total + w
            duo = paired(w)
            wc[l, k * CH : (k + 1) * CH, :] = duo
            row, left = ((k % 3, k < 3), (3 + min(k % 3, 1), k < 5))[k // 3 == 1]
            wp[l, row * CH : (row + 1) * CH, (0 if left else CH) : (CH if left else 2 * CH)] = duo[:, :CH]
        wp[l, 3 * CH : 4 * CH, CH:] = jnp.zeros((CH, CH), BF16)
        psum[...] = total
        return carry

    load_x.wait()
    load_b.wait()
    pl.semaphore_wait(bar, len(around) + 1 + 2 * sides)

    wide = TC + LAY
    half = pl.ds(2 * r, 2)
    mine = pl.ds(pl.multiple_of(LAY * (1 - r), LAY), wide)
    theirs = pl.ds(pl.multiple_of(LAY * r, LAY), wide)
    src_mine = pl.ds(pl.multiple_of((TC - LAY) * r, LAY), wide)
    src_theirs = pl.ds(pl.multiple_of((TC - LAY) * (1 - r), LAY), wide)
    to_core = remote(xin.at[:, src_theirs, :], x0.at[half, theirs, :], s_in.at[0], r_in.at[0], at(sec, 1 - r, c))
    to_right = remote(
        xin.at[:, pl.ds(2 * TC - LAY, LAY), :], x0.at[half, pl.ds(0, LAY), :], s_in.at[1], r_in.at[1 + r], at(sec, 0, c + 1)
    )
    to_left = remote(
        xin.at[:, pl.ds(0, LAY), :], x0.at[half, pl.ds(TW - LAY, LAY), :], s_in.at[2], r_in.at[3 + r], at(sec, 1, c - 1)
    )
    to_core.start()

    @pl.when(c < ncol - 1)
    def _():
        to_right.start()

    @pl.when(c > 0)
    def _():
        to_left.start()

    hrows = pl.ds(pl.multiple_of(r * (CH // 2), CH // 2), CH // 2)
    slab = CH // 8
    prows = pl.ds(pl.multiple_of(slab * (4 * r + c), slab), slab)

    def p_copy(k):
        return remote(
            psum.at[prows, :], pz.at[z, prows, :], s_p.at[k], r_p.at[k], at(x * Z + (z + k) % Z, r, c)
        )

    def y_copy(k):
        part = pz.at[:, prows, :]
        return remote(part, part, s_y.at[k], r_y.at[k], at(sec, r, (c + k) % 4))

    tell(0)
    x0[half, mine, :] = xin[:, src_mine, :]
    lax.fori_loop(0, 4, convert, 0)
    hear(0)
    tell(1)
    lax.fori_loop(4, LAY, convert, 0)
    rows_i = lax.broadcasted_iota(jnp.int32, (CH, CH), 0)
    cols_i = lax.broadcasted_iota(jnp.int32, (CH, CH), 1)
    eye = jnp.where(rows_i == cols_i, 1.0, 0.0).astype(F32)
    psum[...] = eye + STEP * psum[...]
    pz[z, prows, :] = psum[prows, :]
    hear(1)
    tell(2)

    def got_in(i, cols):
        part = x0.at[pl.ds(0, 2), cols, :]
        return remote(part, part, s_in.at[0], r_in.at[i], at(sec, 1 - r, c))

    got_in(0, pl.ds(0, wide)).wait_recv()

    @pl.when((r == 0) & (c > 0))
    def _():
        got_in(1, pl.ds(0, LAY)).wait_recv()
        got_in(2, pl.ds(0, LAY)).wait_recv()

    @pl.when((r == 1) & (c < ncol - 1))
    def _():
        got_in(3, pl.ds(0, LAY)).wait_recv()
        got_in(4, pl.ds(0, LAY)).wait_recv()

    to_core.wait_send()

    @pl.when(c < ncol - 1)
    def _():
        to_right.wait_send()

    @pl.when(c > 0)
    def _():
        to_left.wait_send()

    def set_start(value):
        pad[LAY : LAY + PX, :] = value.reshape(PX, CH)

    def layer(l):
        v = pad[LAY : LAY + PX, :]
        for d in range(3):
            high, low = split(pad[LAY - 1 + d : LAY - 1 + d + PX, :])
            a_buf[0, TW : TW + PX, d * CH : (d + 1) * CH] = high.astype(BF16)
            a_buf[1, TW : TW + PX, d * CH : (d + 1) * CH] = low.astype(BF16)
        rows3 = PX - TW
        pair, third = slice(0, 2 * CH), slice(2 * CH, 3 * CH)
        image, upper = slice(TW, TW + PX), slice(0, PX)

        def dot(a, b):
            return jnp.dot(a, b, preferred_element_type=F32)

        def flat(r):
            return r[:, :CH] + r[:, CH:]

        low_rows = dot(a_buf[1, image, :], wp[l, 0 : 3 * CH, :])
        low_mid = dot(a_buf[1, image, pair], wp[l, 3 * CH : 5 * CH, :])
        beside[0:PX, :] = low_mid[:, CH:]
        mid = jnp.concatenate([a_buf[0, image, pair], a_buf[0, image, third], a_buf[0, upper, third]], axis=1)
        w_mid = jnp.concatenate([wc[l, 3 * CH : 6 * CH, :], wc[l, 2 * CH : 3 * CH, :]], axis=0)
        full = flat(dot(mid, w_mid)) + low_mid[:, :CH] + beside[1 : PX + 1, :]
        above = flat(dot(a_buf[0, TW:PX, pair], wc[l, 0 : 2 * CH, :])) + low_rows[:rows3, :CH]
        below = flat(dot(a_buf[0, 2 * TW : TW + PX, :], wc[l, 6 * CH : 9 * CH, :])) + low_rows[TW:, CH:]
        blank = jnp.zeros((TW, CH), F32)
        pre = full + jnp.concatenate([blank, above], axis=0) + jnp.concatenate([below, blank], axis=0)
        new = (v + STEP * jnp.tanh(pre + bias[pl.ds(l, 1), :])) * mask[...]
        pad[LAY : LAY + PX, :] = new
        return new

    def core(value):
        return value.reshape(H, TW, CH)[:, LAY : LAY + TC, :]

    set_start(x0[...])

    def double(m, carry):
        layer(2 * m)
        layer(2 * m + 1)
        return carry

    def shift(i):
        nxt = sec + 1
        main = remote(cc.at[i], st.at[i, :, pl.ds(LAY, TC), :], s_sh.at[i, 0], r_sh.at[i, 0], at(nxt, r, c))
        rgt = remote(
            cc.at[i, :, pl.ds(TC - LAY, LAY), :], st.at[i, :, pl.ds(0, LAY), :], s_sh.at[i, 1], r_sh.at[i, 1], at(nxt, *right_rc)
        )
        lft = remote(
            cc.at[i, :, pl.ds(0, LAY), :], st.at[i, :, pl.ds(TW - LAY, LAY), :], s_sh.at[i, 2], r_sh.at[i, 2], at(nxt, *left_rc)
        )
        return main, rgt, lft

    def shift_send(i):
        main, rgt, lft = shift(i)

        @pl.when(sec < X * Z - 1)
        def _():
            @pl.when(has_right)
            def _():
                rgt.start()

            @pl.when(has_left)
            def _():
                lft.start()

            main.start()

    def shift_wait(i):
        main, rgt, lft = shift(i)

        @pl.when(sec > 0)
        def _():
            main.wait_recv()

            @pl.when(has_left)
            def _():
                rgt.wait_recv()

            @pl.when(has_right)
            def _():
                lft.wait_recv()

        @pl.when(sec == 0)
        def _():
            st[i] = x0[...]

        @pl.when(sec < X * Z - 1)
        def _():
            main.wait_send()

            @pl.when(has_right)
            def _():
                rgt.wait_send()

            @pl.when(has_left)
            def _():
                lft.wait_send()

    def m_copy(k):
        return remote(mown, mx.at[x], s_m.at[k], r_m.at[k], at(((x + k) % X) * Z + z, r, c))

    def a_copy(i, k):
        j = (z + k) % Z
        part = rs.at[i, j // 2, pl.ds(pl.multiple_of(SH * (j % 2), LAY), SH), :]
        return remote(part, rz.at[i, z], s_a.at[i, k], r_a.at[i, k], at(x * Z + j, 1 - r, c))

    def t_copy(i, k):
        return remote(tb.at[i], tx.at[i, x], s_t.at[i, k], r_t.at[i, k], at(((x + k) % X) * Z + z, r, c))

    my_cols = pl.ds(pl.multiple_of(LAY + SH * (z % 2), LAY), SH)

    def b_copy(i, k):
        j = (z + k) % Z
        return remote(bz.at[i, j], dp.at[i, z // 2, my_cols, :], s_b.at[i, k], r_b.at[i, k], at(x * Z + j, 1 - r, c))

    def h_copy(i, k, side):
        frm = (SH - LAY) if side == 0 else 0
        to = 0 if side == 0 else TW - LAY
        rc = (r, c + 1 - r) if side == 0 else (r, c - r)
        return remote(
            bz.at[i, (z + k) % Z, pl.ds(frm, LAY), :], dp.at[i, z // 2, pl.ds(to, LAY), :], s_h.at[i, k], r_h.at[i, side, z // 2],
            at(x * Z + (z + k) % Z, *rc),
        )

    odd = z % 2 == 1
    own_right, own_left = odd & (2 * c + 1 - r < last), (z % 2 == 0) & (2 * c + 1 - r > 0)
    inner_right, inner_left = odd & (r == 1), (z % 2 == 0) & (r == 0)

    for i in range(CYCLES):
        if i == 0:
            double(0, 0)
            hear(2)
            tell(3)
            for k in (4, 3, 5, 2, 6, 1, 7):
                p_copy(k).start()
            lax.fori_loop(1, LAY // 2, double, 0)
            hear(3)
        else:
            lax.fori_loop(0, LAY // 2, double, 0)
        cc[i] = core(pad[LAY : LAY + PX, :])
        shift_send(i)
        if i == 0:
            for k in range(1, Z):
                p_copy(k).wait()
            for k in (2, 1, 3):
                y_copy(k).start()
        shift_wait(i)
        set_start(st[i])
        lax.fori_loop(0, LAY // 2, double, 0)
        rs[i] = core(pad[LAY : LAY + PX, :]) - cc[i]
        for k in (4, 3, 5, 2, 6, 1, 7, 0):
            a_copy(i, k).start()
        if i == 0:
            for k in range(1, 4):
                y_copy(k).wait()
            forward = remote(pz.at[:, hrows, :], pz.at[:, hrows, :], s_pf.at[0], r_pf.at[0], at(sec, 1 - r, c))
            forward.start()
            forward.wait()
            prefix, suffix = pz[0], eye
            for k in range(Z):
                pc[k] = paired(pz[k])
            for k in range(Z):
                if k > 0:
                    prefix = times(prefix, pc[k])
                if k < Z - 1:
                    qc[:, 2 * CH * k : 2 * CH * (k + 1)] = paired(prefix)
                back = Z - 1 - k
                pair = paired(suffix)
                sc[back * CH : (back + 1) * CH, :] = pair
                if back > 0:
                    suffix = times(pz[back], pair)
            mown[...] = prefix
            for k in range(1, X - 1):
                @pl.when((x >= 1) & (x + k < X))
                def _():
                    m_copy(k).start()
        for k in range(Z):
            a_copy(i, k).wait()
        joined = jnp.concatenate([rz[i, k] for k in range(Z)], axis=1)
        tb[i] = times(joined, sc[...])
        for k in range(1, X):
            t_copy(i, k).start()
        run = rz[i, 0]
        local = [run]
        for k in range(1, Z - 1):
            run = times(run, pc[k]) + rz[i, k]
            local.append(run)
        if i == 0:
            for k in range(1, X - 1):
                @pl.when((x >= 1) & (x + k < X))
                def _():
                    m_copy(k).wait_send()

                @pl.when(x - k >= 1)
                def _():
                    m_copy(k).wait_recv()
            near = mx[jnp.maximum(x - 1, 0)]
            far = mx[jnp.maximum(x - 2, 0)]
            near = jnp.where(x >= 2, near, 0.0)
            far = jnp.where(x >= 3, far, 0.0)
            near_pair = paired(near)
            nc[0:CH, :] = near_pair
            nc[CH : 2 * CH, :] = paired(times(far, near_pair))
        for k in range(1, X):
            t_copy(i, k).wait()
        before = [jnp.where(x >= d, tx[i, jnp.maximum(x - d, 0)], 0.0) for d in range(1, X)]
        carry = before[0] + times(jnp.concatenate(before[1:], axis=1), nc[...])
        bz[i, 0] = carry
        high, low = split(carry)
        spread = jnp.dot(jnp.concatenate([high, low], axis=0).astype(BF16), qc[...], preferred_element_type=F32)
        for k in range(1, Z):
            bz[i, k] = local[k - 1] + fold(spread[:, 2 * CH * (k - 1) : 2 * CH * k], SH)
        for side, sends, inner in ((0, own_right, inner_right), (1, own_left, inner_left)):
            @pl.when(sends)
            def _():
                for k in (4, 3, 5, 2, 6, 1, 7):
                    h_copy(i, k, side).start()

                @pl.when(jnp.logical_not(inner))
                def _():
                    h_copy(i, 0, side).start()

        for k in (4, 3, 5, 2, 6, 1, 7, 0):
            b_copy(i, k).start()

        @pl.when(inner_right)
        def _():
            dp[i, z // 2, 0:LAY, :] = bz[i, z, SH - LAY : SH, :]

        @pl.when(inner_left)
        def _():
            dp[i, z // 2, TW - LAY : TW, :] = bz[i, z, 0:LAY, :]

        for k in range(Z):
            b_copy(i, k).wait()

        def halo_in(side, row):
            part = dp.at[i, row, pl.ds(0 if side == 0 else TW - LAY, LAY), :]
            return remote(part, part, s_h.at[i, 0], r_h.at[i, side, row], at(sec, 1 - r, c))

        if i == CYCLES - 1:
            before = dp[i, :, pl.ds(LAY, TC), :].reshape(H * TC, CH)
            delta = times(before, paired(psum[...])).reshape(H, TC, CH) + rs[i]
            outb[LAY - 1] = cc[i] + delta

        for side, comes, inner in ((0, has_left, inner_right), (1, has_right, inner_left)):
            @pl.when(comes)
            def _():
                for row in range(H):
                    @pl.when(jnp.logical_not(inner & (z // 2 == row)))
                    def _():
                        halo_in(side, row).wait_recv()

        for side, sends, inner in ((0, own_right, inner_right), (1, own_left, inner_left)):
            @pl.when(sends)
            def _():
                for k in range(1, Z):
                    h_copy(i, k, side).wait_send()

                @pl.when(jnp.logical_not(inner))
                def _():
                    h_copy(i, 0, side).wait_send()

        set_start(st[i] + dp[i])

    out_cols = pl.ds(pl.multiple_of(TC * r, LAY), TC)

    def keep(l):
        return pltpu.make_async_copy(outb.at[l, half], out.at[l, 0, :, out_cols, :], l_o.at[l])

    def give(l):
        return remote(
            outb.at[l, pl.ds(2 * (1 - r), 2)], out.at[l, 0, :, out_cols, :], s_o.at[l], r_o.at[l], at(sec, 1 - r, c)
        )

    keep(LAY - 1).start()
    give(LAY - 1).start()

    def final(l, carry):
        outb[l] = core(layer(l))
        keep(l).start()
        give(l).start()
        return carry

    def last_two(m, carry):
        return final(2 * m + 1, final(2 * m, carry))

    lax.fori_loop(0, LAY // 2 - 1, last_two, 0)
    final(LAY - 2, 0)
    for l in range(LAY):
        keep(l).wait()
        give(l).wait()


def shards(inputs, weights, biases):
    V, D = pltpu.VMEM, pltpu.SemaphoreType.DMA
    rows, cols = inputs.shape[1], inputs.shape[2]
    n = CYCLES
    return pl.pallas_call(
        kernel,
        out_shape=jax.ShapeDtypeStruct((LAY,) + inputs.shape, F32),
        in_specs=[
            pl.BlockSpec(memory_space=pltpu.HBM),
            pl.BlockSpec(memory_space=pltpu.HBM),
            pl.BlockSpec(memory_space=pltpu.HBM),
        ],
        out_specs=pl.BlockSpec(memory_space=pl.ANY),
        scratch_shapes=[
            V((rows, cols, CH), F32),
            V((LAY, CH), F32),
            V((H, TW, CH), F32),
            V((LAY, 9, CH, CH), F32),
            V((LAY, 9 * CH, 2 * CH), BF16),
            V((LAY, 5 * CH, 2 * CH), BF16),
            V((PX + LAY, CH), F32),
            V((CH, CH), F32),
            V((2, PX + 2 * TW, 3 * CH), BF16),
            V((PX + 2 * LAY, CH), F32),
            V((PX, CH), F32),
            V((n, H, TW, CH), F32),
            V((n, H, TC, CH), F32),
            V((n, H, TC, CH), F32),
            V((n, Z, SH, CH), F32),
            V((n, Z, SH, CH), F32),
            V((n, H, TW, CH), F32),
            V((n, X, SH, CH), F32),
            V((n, SH, CH), F32),
            V((Z, CH, CH), F32),
            V((X, CH, CH), F32),
            V((CH, CH), F32),
            V((Z, CH, 2 * CH), BF16),
            V((CH, 2 * CH * (Z - 1)), BF16),
            V((Z * CH, 2 * CH), BF16),
            V((2 * CH, 2 * CH), BF16),
            V((LAY, H, TC, CH), F32),
            D((3,)), D((5,)), D((LAY,)), D((n, 3)), D((n, 3)), D((Z,)), D((Z,)), D((1,)), D((1,)),
            D((X,)), D((X,)), D((n, Z)), D((n, Z)), D((n, X)), D((n, X)), D((n, Z)), D((n, Z)),
            D((n, Z)), D((n, 2, H)), D((LAY,)), D((LAY,)), D((LAY,)), D((2,)),
            D((4,)), D((4,)), pltpu.SemaphoreType.REGULAR((4,)),
        ],
        compiler_params=pltpu.CompilerParams(
            collective_id=0, has_side_effects=True, vmem_limit_bytes=54000000
        ),
    )(pltpu.with_memory_space_constraint(inputs, pltpu.HBM), weights, pltpu.with_memory_space_constraint(biases, pltpu.HBM))


def solution(mesh):
    return jax.shard_map(
        shards,
        mesh=mesh,
        in_specs=(P(None, "row", "col", None), P("layer", None, None, None), P("layer", None)),
        out_specs=P("layer", None, "row", "col", None),
        check_vma=False,
    )
```
